16 devices in a mesh: dp: 2 (over y, z), tp: 8 (over x, core).
Axes of the slice: x: 4, y: 2, z: 1, core: 2. Of those that a mesh axis runs over, the one named last changes fastest.
The devices are a block of a 4x4x8 slice.
Arguments:
- tokens: int32 [96], P('dp'), parts along dimension 0
- positions: int32 [96], P('dp'), parts along dimension 0
- self_keys: bfloat16 [2, 96, 448, 8, 64], P(None, 'dp', None, 'tp'), parts along dimension 1
- self_vals: bfloat16 [2, 96, 448, 8, 64], P(None, 'dp', None, 'tp'), parts along dimension 1
- cross_keys: bfloat16 [2, 96, 1500, 8, 64], P(None, 'dp', None, 'tp'), parts along dimension 1
- cross_vals: bfloat16 [2, 96, 1500, 8, 64], P(None, 'dp', None, 'tp'), parts along dimension 1
- embed_table: bfloat16 [52224, 512], P('tp')
- pos_table: bfloat16 [448, 512], replicated
- w_qkv: bfloat16 [2, 512, 3, 8, 64], P(None, None, None, 'tp')
- w_cq: bfloat16 [2, 512, 8, 64], P(None, None, 'tp')
- in_bias: float32 [2, 3, 8, 64], P(None, None, 'tp')
- w_out: bfloat16 [2, 2, 8, 64, 512], P(None, None, 'tp')
- out_bias: float32 [2, 3, 512], replicated
- w_fc1: bfloat16 [2, 512, 2048], P(None, None, 'tp')
- b_fc1: float32 [2, 2048], P(None, 'tp')
- w_fc2: bfloat16 [2, 2048, 512], P(None, 'tp')
- ln_layers: float32 [2, 3, 2, 512], replicated
- ln_final: float32 [2, 512], replicated
Outputs:
- output 1: float32 [96, 52224], P('dp', 'tp'), parts along dimension 0
- output 2: bfloat16 [2, 96, 448, 8, 64], P(None, 'dp', None, 'tp'), parts along dimension 1
- output 3: bfloat16 [2, 96, 448, 8, 64], P(None, 'dp', None, 'tp'), parts along dimension 1
There are 2 independent parts. The reference program is written for one: setup_inputs(seed, part) draws one part's arguments, and reference() takes and returns one part's arrays. A program takes and returns all parts, laid end to end along the dimension named above; an argument that names none is the same for every part.
All inputs are finite; a program needn't handle non-finite values.
Results may differ from the reference program's by a relative error of at most 0.0123317.
Values are sent between devices in bfloat16 or wider.
A program may use at most 768 MiB of HBM per device.

```python
import jax
import jax.numpy as jnp
from jax import lax

SEQ_BATCH = 48
D_MODEL = 512
N_HEADS = 8
HEAD_DIM = 64
FF_DIM = 2048
VOCAB_SIZE = 51865
VOCAB_PAD = 52224
TEXT_CTX = 448
FRAMES = 1500
LAYERS = 2
FRAME_RANK = 8


def setup_inputs(seed: int = 0, part: int = 0) -> dict:
    base_key = jax.random.key(seed)
    part_keys = jax.random.split(jax.random.fold_in(base_key, part), 12)
    shared_keys = jax.random.split(jax.random.fold_in(base_key, 1000003), 14)

    def normal_draw(key_in, draw_shape, factor):
        return jax.random.normal(key_in, draw_shape, jnp.float32) * factor

    def structured(code_key, basis_key, noise_key, length, factor, noise_std):
        frame_codes = normal_draw(code_key, (SEQ_BATCH, length, FRAME_RANK), 1.0)
        code_basis = normal_draw(basis_key, (LAYERS, SEQ_BATCH, FRAME_RANK, N_HEADS, HEAD_DIM), factor * FRAME_RANK ** -0.5)
        mixed_rows = jnp.einsum('btr,lbrhe->lbthe', frame_codes, code_basis)
        return mixed_rows + normal_draw(noise_key, (LAYERS, SEQ_BATCH, length, N_HEADS, HEAD_DIM), noise_std)

    tokens = jax.random.randint(part_keys[0], (SEQ_BATCH,), 0, VOCAB_SIZE, dtype=jnp.int32)
    tokens = tokens.at[0].set(VOCAB_SIZE - 1).at[1].set(0)
    positions = jax.random.randint(part_keys[1], (SEQ_BATCH,), 0, TEXT_CTX, dtype=jnp.int32)
    positions = positions.at[0].set(TEXT_CTX - 1).at[1].set(0)
    self_keys = structured(part_keys[2], part_keys[3], part_keys[4], TEXT_CTX, 1.0, 0.3).astype(jnp.bfloat16)
    self_vals = structured(part_keys[2], part_keys[5], part_keys[6], TEXT_CTX, 1.0, 0.5).astype(jnp.bfloat16)
    cross_keys = structured(part_keys[7], part_keys[8], part_keys[9], FRAMES, 1.0, 0.3).astype(jnp.bfloat16)
    cross_vals = structured(part_keys[7], part_keys[10], part_keys[11], FRAMES, 1.0, 0.5).astype(jnp.bfloat16)
    embed_table = normal_draw(shared_keys[12], (VOCAB_PAD, D_MODEL), D_MODEL ** -0.25).astype(jnp.bfloat16)
    pos_table = normal_draw(shared_keys[13], (TEXT_CTX, D_MODEL), 0.5).astype(jnp.bfloat16)
    w_qkv = normal_draw(shared_keys[0], (LAYERS, D_MODEL, 3, N_HEADS, HEAD_DIM), D_MODEL ** -0.5).astype(jnp.bfloat16)
    w_cq = normal_draw(shared_keys[1], (LAYERS, D_MODEL, N_HEADS, HEAD_DIM), D_MODEL ** -0.5).astype(jnp.bfloat16)
    in_bias = normal_draw(shared_keys[2], (LAYERS, 3, N_HEADS, HEAD_DIM), 0.3)
    w_out = normal_draw(shared_keys[3], (LAYERS, 2, N_HEADS, HEAD_DIM, D_MODEL), D_MODEL ** -0.5).astype(jnp.bfloat16)
    out_bias = normal_draw(shared_keys[4], (LAYERS, 3, D_MODEL), 0.3)
    w_fc1 = normal_draw(shared_keys[5], (LAYERS, D_MODEL, FF_DIM), D_MODEL ** -0.5).astype(jnp.bfloat16)
    b_fc1 = normal_draw(shared_keys[6], (LAYERS, FF_DIM), 0.3)
    w_fc2 = normal_draw(shared_keys[7], (LAYERS, FF_DIM, D_MODEL), FF_DIM ** -0.5).astype(jnp.bfloat16)
    ln_layers = jnp.concatenate([1.0 + normal_draw(shared_keys[8], (LAYERS, 3, 1, D_MODEL), 0.2), normal_draw(shared_keys[9], (LAYERS, 3, 1, D_MODEL), 0.2)], axis=2)
    ln_final = jnp.concatenate([1.0 + normal_draw(shared_keys[10], (1, D_MODEL), 0.2), normal_draw(shared_keys[11], (1, D_MODEL), 0.2)], axis=0)
    return {'tokens': tokens, 'positions': positions, 'self_keys': self_keys, 'self_vals': self_vals, 'cross_keys': cross_keys, 'cross_vals': cross_vals, 'embed_table': embed_table, 'pos_table': pos_table, 'w_qkv': w_qkv, 'w_cq': w_cq, 'in_bias': in_bias, 'w_out': w_out, 'out_bias': out_bias, 'w_fc1': w_fc1, 'b_fc1': b_fc1, 'w_fc2': w_fc2, 'ln_layers': ln_layers, 'ln_final': ln_final}


def layer_norm(resid_in, ln_gain, ln_shift):
    row_mean = jnp.mean(resid_in, axis=-1, keepdims=True)
    centred = resid_in - row_mean
    variance = jnp.mean(centred * centred, axis=-1, keepdims=True)
    return (centred * lax.rsqrt(variance + 1e-5) * ln_gain + ln_shift).astype(jnp.bfloat16)


def attend(queries, key_rows, val_rows, mask_add):
    scores = jnp.einsum('bhe,bthe->bht', queries.astype(jnp.float32), key_rows.astype(jnp.float32)) * (HEAD_DIM ** -0.5) + mask_add
    weights = jax.nn.softmax(scores, axis=-1).astype(jnp.bfloat16)
    mixed_vals = jnp.einsum('bht,bthe->bhe', weights.astype(jnp.float32), val_rows.astype(jnp.float32))
    return mixed_vals.astype(jnp.bfloat16)


def project_out(attended, out_weight):
    summed = jnp.einsum('bhe,hed->bd', attended.astype(jnp.float32), out_weight.astype(jnp.float32))
    return summed.astype(jnp.bfloat16).astype(jnp.float32)


def reference(tokens, positions, self_keys, self_vals, cross_keys, cross_vals, embed_table, pos_table, w_qkv, w_cq, in_bias, w_out, out_bias, w_fc1, b_fc1, w_fc2, ln_layers, ln_final):
    residual = embed_table[tokens].astype(jnp.float32) + pos_table[positions].astype(jnp.float32)
    cache_pos = jnp.arange(TEXT_CTX)[None, :]
    write_mask = (cache_pos == positions[:, None])[:, :, None, None]
    self_mask = jnp.where(cache_pos <= positions[:, None], 0.0, -1e30)[:, None, :]

    def layer_body(resid_in, layer_args):
        (cache_keys, cache_vals, frame_keys, frame_vals, qkv_weight, cq_weight, bias_in, out_weight, bias_out, fc1_weight, fc1_bias, fc2_weight, ln_params) = layer_args
        hidden = layer_norm(resid_in, ln_params[0, 0], ln_params[0, 1])
        projected = jnp.einsum('bd,dthe->bthe', hidden.astype(jnp.float32), qkv_weight.astype(jnp.float32))
        queries = (projected[:, 0] + bias_in[0]).astype(jnp.bfloat16)
        key_new = projected[:, 1].astype(jnp.bfloat16)
        val_new = (projected[:, 2] + bias_in[1]).astype(jnp.bfloat16)
        keys_now = jnp.where(write_mask, key_new[:, None], cache_keys)
        vals_now = jnp.where(write_mask, val_new[:, None], cache_vals)
        resid_mid = resid_in + project_out(attend(queries, keys_now, vals_now, self_mask), out_weight[0]) + bias_out[0]
        hidden = layer_norm(resid_mid, ln_params[1, 0], ln_params[1, 1])
        cross_q = (jnp.einsum('bd,dhe->bhe', hidden.astype(jnp.float32), cq_weight.astype(jnp.float32)) + bias_in[2]).astype(jnp.bfloat16)
        resid_mid = resid_mid + project_out(attend(cross_q, frame_keys, frame_vals, 0.0), out_weight[1]) + bias_out[1]
        hidden = layer_norm(resid_mid, ln_params[2, 0], ln_params[2, 1])
        fc1_out = jnp.dot(hidden, fc1_weight, preferred_element_type=jnp.float32) + fc1_bias
        active = jax.nn.gelu(fc1_out, approximate=False).astype(jnp.bfloat16)
        fc2_out = jnp.dot(active, fc2_weight, preferred_element_type=jnp.float32).astype(jnp.bfloat16).astype(jnp.float32)
        resid_out = resid_mid + fc2_out + bias_out[2]
        return resid_out, (keys_now, vals_now)

    residual, new_caches = lax.scan(layer_body, residual, (self_keys, self_vals, cross_keys, cross_vals, w_qkv, w_cq, in_bias, w_out, out_bias, w_fc1, b_fc1, w_fc2, ln_layers))
    final_hidden = layer_norm(residual, ln_final[0], ln_final[1])
    logits = jnp.dot(final_hidden, embed_table.T, preferred_element_type=jnp.float32)
    return logits, new_caches[0], new_caches[1]
```

```python
import functools

import jax
import jax.numpy as jnp
from jax import lax
from jax.experimental import pallas as pl
from jax.experimental.pallas import tpu as pltpu
from jax.sharding import PartitionSpec as P

MESH = pl.DeviceIdType.MESH
GROUP = 16
F32 = jnp.float32
BF16 = jnp.bfloat16
NT = (((1,), (1,)), ((), ()))


def dot_nt(a, b):
    return lax.dot_general(a, b, NT, preferred_element_type=F32)


def dot_nn(a, b):
    return jnp.dot(a, b, preferred_element_type=F32)


def layer_norm(x, gain, shift):
    mean = jnp.mean(x, axis=-1, keepdims=True)
    centred = x - mean
    variance = jnp.mean(centred * centred, axis=-1, keepdims=True)
    return (centred * lax.rsqrt(variance + 1e-5) * gain + shift).astype(BF16)


def step_kernel(
    n, emb, pos_rows, positions, w_qkv, w_cq, in_bias, out_bias, fc1, b_fc1, ln_layers, ln_final, w_out, fc2,
    self_k, self_v, cross_k, cross_v,
    final_out, knew_out, vnew_out,
    sk, sv, ck, cv, wo_full, fc2_full, emb_slots, o_slots, act_slots, q_bd, scores,
    sem_sk, sem_sv, sem_ck, sem_cv, sem_w, emb_send, emb_recv, o_send, o_recv, act_send, act_recv, w_send, w_recv,
):
    layers, batch = sk.shape[0], emb.shape[0]
    head = w_cq.shape[1]
    span = GROUP * head
    me = lax.axis_index("tp")
    partner = me + 1 - 2 * lax.rem(me, 2)

    def peer(k):
        return lax.rem(me + k, n)

    barrier = pltpu.get_barrier_semaphore()
    for k in range(1, n):
        pl.semaphore_signal(barrier, 1, device_id={"tp": peer(k)}, device_id_type=MESH)
    pl.semaphore_wait(barrier, n - 1)

    def remote(src, dst, send, recv, to):
        return pltpu.make_async_remote_copy(src, dst, send, recv, device_id={"tp": to}, device_id_type=MESH)

    order = sorted(range(1, n), key=lambda k: -min(k, n - k))

    def send_all(src, slots, send, recv):
        copies = [remote(src, slots.at[me], send.at[k], recv.at[me], peer(k)) for k in order]
        for c in copies:
            c.start()
        return copies

    def wait_all(copies, src, slots, send, recv):
        for k in order:
            j = peer(k)
            remote(src, slots.at[j], send.at[k], recv.at[j], j).wait_recv()
        for c in copies:
            c.wait_send()

    wo_parts = [(w_out.at[l, a], wo_full.at[l, a]) for l in range(layers) for a in range(2)]
    fc2_parts = [(fc2.at[l], fc2_full.at[l]) for l in range(layers)]
    parts = [wo_parts[0], wo_parts[1], fc2_parts[0], wo_parts[2], wo_parts[3], fc2_parts[1]]
    own_copies, first_hop, second_hop = {}, {}, {}

    def weights_start(i):
        src, full = parts[i]
        own_copies[i] = pltpu.make_async_copy(src, full.at[me], sem_w.at[i])
        own_copies[i].start()
        first_hop[i] = [remote(src, full.at[me], w_send.at[i, k], w_recv.at[i, me], peer(k)) for k in range(2, n, 2)]
        first_hop[i].append(remote(src, full.at[me], w_send.at[i, 1], w_recv.at[i, me], partner))
        for c in first_hop[i]:
            c.start()

    def weights_forward(i):
        src, full = parts[i]
        second_hop[i] = []
        for k in range(2, n, 2):
            j = peer(k)
            remote(src, full.at[j], w_send.at[i, k], w_recv.at[i, j], j).wait_recv()
            c = remote(full.at[j], full.at[j], w_send.at[i, k + 1], w_recv.at[i, j], partner)
            c.start()
            second_hop[i].append(c)

    def weights_wait(i):
        src, full = parts[i]
        remote(src, full.at[partner], w_send.at[i, 1], w_recv.at[i, partner], partner).wait_recv()
        for k in range(2, n, 2):
            j = lax.rem(partner + k, n)
            remote(src, full.at[j], w_send.at[i, k + 1], w_recv.at[i, j], partner).wait_recv()
        for c in first_hop[i] + second_hop[i]:
            c.wait_send()
        own_copies[i].wait()

    emb_copies = send_all(emb, emb_slots, emb_send, emb_recv)
    weights_start(0)

    loads = {}
    for l in range(layers):
        for name, src, dst, sem in (("sk", self_k, sk, sem_sk), ("sv", self_v, sv, sem_sv), ("ck", cross_k, ck, sem_ck), ("cv", cross_v, cv, sem_cv)):
            loads[name, l] = pltpu.make_async_copy(src.at[l], dst.at[l], sem.at[l])
            loads[name, l].start()
    weights_start(1)

    emb_slots[me] = emb[...]
    wait_all(emb_copies, emb, emb_slots, emb_send, emb_recv)
    x = emb_slots[0].astype(F32)
    for j in range(1, n):
        x = x + emb_slots[j].astype(F32)
    x = x + pos_rows[...].astype(F32)

    row = lax.broadcasted_iota(jnp.int32, (batch, span), 0)
    col = lax.broadcasted_iota(jnp.int32, (batch, span), 1)
    diagonal = lax.rem(row, GROUP) == lax.div(col, head)
    group_diagonal = diagonal[:GROUP]

    def attend(q, keys, vals, finish):
        length = keys.shape[2]
        wide = jnp.concatenate([q] * GROUP, axis=1)
        q_bd[...] = jnp.where(diagonal, wide, 0).astype(BF16)
        for g in range(batch // GROUP):
            rows = slice(g * GROUP, (g + 1) * GROUP)
            scores[rows, :length] = dot_nn(q_bd[rows], keys[rows].reshape(span, length))
        weights, extra = finish(scores[:, :length] * (head ** -0.5))
        out = []
        for g in range(batch // GROUP):
            rows = slice(g * GROUP, (g + 1) * GROUP)
            full = dot_nt(weights[rows], vals[rows].reshape(span, length))
            full = jnp.where(group_diagonal, full, 0.0)
            while full.shape[1] > head:
                half = full.shape[1] // 2
                full = full[:, :half] + full[:, half:]
            out.append(full)
        return jnp.concatenate(out, axis=0) + extra

    def exchange_heads(e, attended):
        slots, send, recv = o_slots.at[e], o_send.at[e], o_recv.at[e]
        slots[me] = attended
        return send_all(slots.at[me], slots, send, recv)

    def gathered_heads(e, copies):
        slots, send, recv = o_slots.at[e], o_send.at[e], o_recv.at[e]
        wait_all(copies, slots.at[me], slots, send, recv)
        return jnp.concatenate([slots[j] for j in range(n)], axis=1)

    def project(heads, w, bias):
        return dot_nn(heads, w[...].reshape(n * head, -1)).astype(BF16).astype(F32), bias

    for l in range(layers):
        ln = ln_layers[l]
        h = layer_norm(x, ln[0, 0:1], ln[0, 1:2])
        q = (dot_nt(h, w_qkv[l, 0]) + in_bias[l, 0:1]).astype(BF16)
        k_new = dot_nt(h, w_qkv[l, 1]).astype(BF16)
        v_new = (dot_nt(h, w_qkv[l, 2]) + in_bias[l, 1:2]).astype(BF16)
        knew_out[l] = k_new
        vnew_out[l] = v_new
        loads["sk", l].wait()
        loads["sv", l].wait()
        new_score = jnp.sum(q.astype(F32) * k_new.astype(F32), axis=-1, keepdims=True) * (head ** -0.5)

        def finish_self(s):
            place = lax.broadcasted_iota(jnp.int32, s.shape, 1)
            s = jnp.where(place < positions[...], s, -1e30)
            peak = jnp.maximum(jnp.max(s, axis=-1, keepdims=True), new_score)
            e = jnp.exp(s - peak)
            e_new = jnp.exp(new_score - peak)
            total = jnp.sum(e, axis=-1, keepdims=True) + e_new
            return (e / total).astype(BF16), (e_new / total).astype(BF16).astype(F32) * v_new.astype(F32)

        def finish_cross(s):
            e = jnp.exp(s - jnp.max(s, axis=-1, keepdims=True))
            return (e / jnp.sum(e, axis=-1, keepdims=True)).astype(BF16), 0.0

        attended = attend(q, sk.at[l], sv.at[l], finish_self).astype(BF16)
        copies = exchange_heads(2 * l, attended)
        weights_start(3 * l + 2)
        weights_forward(3 * l)
        weights_wait(3 * l)
        heads = gathered_heads(2 * l, copies)
        x = x + dot_nn(heads, wo_full[l, 0].reshape(n * head, -1)).astype(BF16).astype(F32) + out_bias[l, 0:1]

        h = layer_norm(x, ln[1, 0:1], ln[1, 1:2])
        q = (dot_nt(h, w_cq[l]) + in_bias[l, 2:3]).astype(BF16)
        loads["ck", l].wait()
        loads["cv", l].wait()
        attended = attend(q, ck.at[l], cv.at[l], finish_cross).astype(BF16)
        copies = exchange_heads(2 * l + 1, attended)
        weights_forward(3 * l + 1)
        weights_wait(3 * l + 1)
        heads = gathered_heads(2 * l + 1, copies)
        x = x + dot_nn(heads, wo_full[l, 1].reshape(n * head, -1)).astype(BF16).astype(F32) + out_bias[l, 1:2]

        h = layer_norm(x, ln[2, 0:1], ln[2, 1:2])
        hidden = dot_nn(h, fc1[l]) + b_fc1[l : l + 1]
        active = (0.5 * hidden * (1.0 + lax.erf(hidden * (0.5 ** 0.5)))).astype(BF16)
        slots, send, recv = act_slots.at[l], act_send.at[l], act_recv.at[l]
        slots[me] = active
        copies = send_all(slots.at[me], slots, send, recv)
        weights_forward(3 * l + 2)
        weights_wait(3 * l + 2)
        if l + 1 < layers:
            weights_start(3 * l + 3)
            weights_start(3 * l + 4)
        wait_all(copies, slots.at[me], slots, send, recv)
        total = dot_nn(slots[0], fc2_full[l, 0])
        for j in range(1, n):
            total = total + dot_nn(slots[j], fc2_full[l, j])
        x = x + total.astype(BF16).astype(F32) + out_bias[l, 2:3]

    final_out[...] = layer_norm(x, ln_final[0:1], ln_final[1:2])


def solution(mesh):
    n = mesh.shape["tp"]

    def local_step(tokens, positions, self_keys, self_vals, cross_keys, cross_vals, embed_table, pos_table, w_qkv, w_cq, in_bias, w_out, out_bias, w_fc1, b_fc1, w_fc2, ln_layers, ln_final):
        layers, batch, ctx, _, head = self_keys.shape
        frames = cross_keys.shape[2]
        width = embed_table.shape[1]
        hidden = w_fc1.shape[2]
        shard_rows = embed_table.shape[0]
        local_ids = tokens - lax.axis_index("tp") * shard_rows
        owned = (local_ids >= 0) & (local_ids < shard_rows)
        picked = jnp.take(embed_table, jnp.clip(local_ids, 0, shard_rows - 1), axis=0)
        picked = jnp.where(owned[:, None], picked, jnp.zeros_like(picked))
        pos_rows = jnp.take(pos_table, positions, axis=0)

        def by_place(cache):
            return jnp.transpose(cache[:, :, :, 0, :], (0, 1, 3, 2))

        vmem = pl.BlockSpec(memory_space=pltpu.VMEM)
        hbm = pl.BlockSpec(memory_space=pl.ANY)
        rows = jax.ShapeDtypeStruct((layers, batch, head), BF16)
        final_hidden, k_new, v_new = pl.pallas_call(
            functools.partial(step_kernel, n),
            out_shape=(jax.ShapeDtypeStruct((batch, width), BF16), rows, rows),
            in_specs=[vmem] * 11 + [hbm] * 6,
            out_specs=(vmem, vmem, vmem),
            scratch_shapes=[
                pltpu.VMEM((layers, batch, head, ctx), BF16),
                pltpu.VMEM((layers, batch, head, ctx), BF16),
                pltpu.VMEM((layers, batch, head, frames), BF16),
                pltpu.VMEM((layers, batch, head, frames), BF16),
                pltpu.VMEM((layers, 2, n, head, width), BF16),
                pltpu.VMEM((layers, n, hidden, width), BF16),
                pltpu.VMEM((n, batch, width), BF16),
                pltpu.VMEM((2 * layers, n, batch, head), BF16),
                pltpu.VMEM((layers, n, batch, hidden), BF16),
                pltpu.VMEM((batch, GROUP * head), BF16),
                pltpu.VMEM((batch, frames), F32),
                pltpu.SemaphoreType.DMA((layers,)),
                pltpu.SemaphoreType.DMA((layers,)),
                pltpu.SemaphoreType.DMA((layers,)),
                pltpu.SemaphoreType.DMA((layers,)),
                pltpu.SemaphoreType.DMA((3 * layers,)),
                pltpu.SemaphoreType.DMA((n,)),
                pltpu.SemaphoreType.DMA((n,)),
                pltpu.SemaphoreType.DMA((2 * layers, n)),
                pltpu.SemaphoreType.DMA((2 * layers, n)),
                pltpu.SemaphoreType.DMA((layers, n)),
                pltpu.SemaphoreType.DMA((layers, n)),
                pltpu.SemaphoreType.DMA((3 * layers, n)),
                pltpu.SemaphoreType.DMA((3 * layers, n)),
            ],
            compiler_params=pltpu.CompilerParams(collective_id=0, has_side_effects=True, vmem_limit_bytes=63 * 1024 * 1024),
            name="decode_step",
        )(
            picked, pos_rows, positions[:, None],
            jnp.transpose(w_qkv[:, :, :, 0, :], (0, 2, 3, 1)), jnp.transpose(w_cq[:, :, 0, :], (0, 2, 1)), in_bias[:, :, 0, :],
            out_bias, w_fc1, b_fc1, ln_layers, ln_final, w_out[:, :, 0], w_fc2,
            by_place(self_keys), by_place(self_vals), by_place(cross_keys), by_place(cross_vals),
        )
        logits = jnp.einsum("bd,vd->bv", final_hidden, embed_table, preferred_element_type=F32)
        write_mask = (jnp.arange(ctx)[None, :] == positions[:, None])[None, :, :, None, None]
        new_keys = jnp.where(write_mask, k_new[:, :, None, None, :], self_keys)
        new_vals = jnp.where(write_mask, v_new[:, :, None, None, :], self_vals)
        return logits, new_keys, new_vals

    batch_spec = P("dp")
    cache_spec = P(None, "dp", None, "tp", None)
    in_specs = (batch_spec, batch_spec, cache_spec, cache_spec, cache_spec, cache_spec, P("tp", None), P(None, None), P(None, None, None, "tp", None), P(None, None, "tp", None), P(None, None, "tp", None), P(None, None, "tp", None, None), P(None, None, None), P(None, None, "tp"), P(None, "tp"), P(None, "tp", None), P(None, None, None, None), P(None, None))
    out_specs = (P("dp", "tp"), cache_spec, cache_spec)
    return jax.shard_map(local_step, mesh=mesh, in_specs=in_specs, out_specs=out_specs, check_vma=False)
```

```python
import functools

import jax
import jax.numpy as jnp
from jax import lax
from jax.experimental import pallas as pl
from jax.experimental.pallas import tpu as pltpu
from jax.sharding import PartitionSpec as P

MESH = pl.DeviceIdType.MESH
GROUP = 16
LANES = 128
CHUNKS = 8
STEP_VMEM = 42 * 1024 * 1024
LAST_VMEM = 8 * 1024 * 1024
F32 = jnp.float32
BF16 = jnp.bfloat16
NT = (((1,), (1,)), ((), ()))


def dot_nt(a, b):
    return lax.dot_general(a, b, NT, preferred_element_type=F32)


def dot_nn(a, b):
    return jnp.dot(a, b, preferred_element_type=F32)


def layer_norm(x, gain, shift):
    mean = jnp.mean(x, axis=-1, keepdims=True)
    centred = x - mean
    variance = jnp.mean(centred * centred, axis=-1, keepdims=True)
    return (centred * lax.rsqrt(variance + 1e-5) * gain + shift).astype(BF16)


def step_kernel(
    n, tokens, positions, in_bias, out_bias, b_fc1, ln_layers, ln_final,
    embed, pos_table, w_qkv_hbm, w_cq_hbm, fc1_hbm, fc2_hbm, w_out, self_k, self_v, cross_k, cross_v,
    final_out, table, sk, sv,
    ck, cv, wo_full, pos_vmem, w_qkv, w_cq, fc1, fc2, emb_own, emb_partner, emb_chip, emb_slots, o_slots,
    rs_src, rs_slots, ag_slots, q_bd, scores, one_hot, columns,
    sem_e, sem_p, sem_own, sem_self, sem_cross, sem_w, pair_send, pair_recv, emb_send, emb_recv,
    o_send, o_recv, rs_send, rs_recv, ag_send, ag_recv, w_send, w_recv,
):
    layers, batch = sk.shape[0], sk.shape[1]
    head, ctx = sk.shape[2], sk.shape[3]
    width = table.shape[1]
    half, block = batch // 2, width // (n // 2)
    span = GROUP * head
    me = lax.axis_index("tp")
    core, chip = lax.rem(me, 2), lax.div(me, 2)
    partner = me + 1 - 2 * core

    def peer(k):
        return lax.rem(me + k, n)

    chunks = sem_e.shape[0]
    chunk = table.shape[0] // chunks
    table_loads = [pltpu.make_async_copy(embed.at[pl.ds(c * chunk, chunk)], table.at[pl.ds(c * chunk, chunk)], sem_e.at[c]) for c in range(chunks)]
    for c in table_loads:
        c.start()
    pos_load = pltpu.make_async_copy(pos_table, pos_vmem, sem_p)
    pos_load.start()
    own = [pltpu.make_async_copy(a, b, sem_own.at[i]) for i, (a, b) in enumerate(((w_qkv_hbm, w_qkv), (w_cq_hbm, w_cq), (fc1_hbm, fc1), (fc2_hbm, fc2)))]
    own[0].start()
    self_loads = [[pltpu.make_async_copy(a.at[l], b.at[l], sem_self.at[l, i]) for i, (a, b) in enumerate(((self_k, sk), (self_v, sv)))] for l in range(layers)]
    key_loads = [pltpu.make_async_copy(cross_k.at[l], ck.at[l], sem_cross.at[l, 0]) for l in range(layers)]
    val_loads = [pltpu.make_async_copy(cross_v.at[l], cv, sem_cross.at[l, 1]) for l in range(layers)]
    for c in self_loads[0]:
        c.start()
    for c in own[1:]:
        c.start()
    key_loads[0].start()
    val_loads[0].start()
    for l in range(1, layers):
        for c in self_loads[l]:
            c.start()
        key_loads[l].start()

    barrier = pltpu.get_barrier_semaphore()
    for k in range(1, n):
        pl.semaphore_signal(barrier, 1, device_id={"tp": peer(k)}, device_id_type=MESH)

    def remote(src, dst, send, recv, to):
        return pltpu.make_async_remote_copy(src, dst, send, recv, device_id={"tp": to}, device_id_type=MESH)

    order = sorted(range(1, n), key=lambda k: -min(k, n - k))

    def send_all(src_of, slots, send, recv):
        copies = [remote(src_of(peer(k)), slots.at[me], send.at[k], recv.at[me], peer(k)) for k in order]
        for c in copies:
            c.start()
        return copies

    def wait_all(copies, slots, send, recv):
        for k in order:
            j = peer(k)
            remote(slots.at[j], slots.at[j], send.at[k], recv.at[j], j).wait_recv()
        for c in copies:
            c.wait_send()

    parts = [(w_out.at[l, a], wo_full.at[l, a]) for l in range(layers) for a in range(2)]
    own_copies, first_hop, second_hop = {}, {}, {}

    def weights_start(i):
        src, full = parts[i]
        own_copies[i] = pltpu.make_async_copy(src, full.at[me], sem_w.at[i])
        own_copies[i].start()
        first_hop[i] = [remote(src, full.at[me], w_send.at[i, k], w_recv.at[i, me], peer(k)) for k in range(2, n, 2)]
        first_hop[i].append(remote(src, full.at[me], w_send.at[i, 1], w_recv.at[i, me], partner))
        for c in first_hop[i]:
            c.start()

    def weights_forward(i):
        src, full = parts[i]
        second_hop[i] = []
        for k in range(2, n, 2):
            j = peer(k)
            remote(src, full.at[j], w_send.at[i, k], w_recv.at[i, j], j).wait_recv()
            c = remote(full.at[j], full.at[j], w_send.at[i, k + 1], w_recv.at[i, j], partner)
            c.start()
            second_hop[i].append(c)

    def weights_wait(i):
        src, full = parts[i]
        remote(src, full.at[partner], w_send.at[i, 1], w_recv.at[i, partner], partner).wait_recv()
        for k in range(2, n, 2):
            j = lax.rem(partner + k, n)
            remote(src, full.at[j], w_send.at[i, k + 1], w_recv.at[i, j], partner).wait_recv()
        for c in first_hop[i] + second_hop[i]:
            c.wait_send()
        own_copies[i].wait()

    def as_column(row):
        i = lax.broadcasted_iota(jnp.int32, (batch, batch), 0)
        j = lax.broadcasted_iota(jnp.int32, (batch, batch), 1)
        return jnp.sum(jnp.where(i == j, jnp.broadcast_to(row.astype(F32), (batch, batch)), 0.0), axis=1, keepdims=True)

    token = as_column(tokens[...]).astype(jnp.int32) - me * table.shape[0]
    place = as_column(positions[...]).astype(jnp.int32)
    picked = jnp.zeros((batch, width), F32)
    for c in range(chunks):
        table_loads[c].wait()
        hit = lax.broadcasted_iota(jnp.int32, (batch, chunk), 1) + c * chunk == token
        picked = picked + dot_nn(jnp.where(hit, 1.0, 0.0).astype(BF16), table[c * chunk : (c + 1) * chunk])
    emb_own[...] = picked.astype(BF16)

    pl.semaphore_wait(barrier, n - 1)
    pair = remote(emb_own, emb_partner, pair_send, pair_recv, partner)
    pair.start()
    hit = lax.broadcasted_iota(jnp.int32, (batch, ctx), 1) == place
    hit = jnp.where(hit, 1.0, 0.0)
    for t in range(0, ctx, LANES):
        size = min(LANES, ctx - t)
        one_hot[t // LANES, :, :size] = hit[:, t : t + size]
    pos_load.wait()
    pos_rows = dot_nn(hit.astype(BF16), pos_vmem[...])
    pair.wait()
    pair_sum = picked + emb_partner[...].astype(F32)
    for r in range(2):
        emb_chip[r] = pair_sum[r * half : (r + 1) * half].astype(BF16)
    others = [k for k in order]
    sends = []
    for dc in (n // 4, *[d for d in range(1, n // 2) if d != n // 4]):
        for other in range(2):
            to = lax.rem(chip + dc, n // 2) * 2 + lax.rem(core + other, 2)
            sends.append(remote(emb_chip.at[core], emb_slots.at[chip, core], emb_send.at[dc, other], emb_recv.at[chip, core], to))
    for c in sends:
        c.start()
    weights_start(0)
    x_parts = [pair_sum[r * half : (r + 1) * half] for r in range(2)]
    for dc in range(1, n // 2):
        far = lax.rem(chip + dc, n // 2)
        for r in range(2):
            remote(emb_chip.at[0], emb_slots.at[far, r], emb_send.at[dc, r], emb_recv.at[far, r], far * 2 + r).wait_recv()
            x_parts[r] = x_parts[r] + emb_slots[far, r].astype(F32)
    for c in sends:
        c.wait_send()
    x = jnp.concatenate(x_parts, axis=0) + pos_rows

    row = lax.broadcasted_iota(jnp.int32, (batch, span), 0)
    col = lax.broadcasted_iota(jnp.int32, (batch, span), 1)
    diagonal = lax.rem(row, GROUP) == lax.div(col, head)
    group_diagonal = diagonal[:GROUP]

    def attend(q, keys, vals, finish):
        length = keys.shape[2]
        wide = jnp.concatenate([q] * GROUP, axis=1)
        q_bd[...] = jnp.where(diagonal, wide, 0).astype(BF16)
        for g in range(batch // GROUP):
            rows = slice(g * GROUP, (g + 1) * GROUP)
            scores[rows, :length] = dot_nn(q_bd[rows], keys[rows].reshape(span, length))
        weights, extra = finish(scores[:, :length] * (head ** -0.5))
        out = []
        for g in range(batch // GROUP):
            rows = slice(g * GROUP, (g + 1) * GROUP)
            full = dot_nt(weights[rows], vals[rows].reshape(span, length))
            full = jnp.where(group_diagonal, full, 0.0)
            while full.shape[1] > head:
                mid = full.shape[1] // 2
                full = full[:, :mid] + full[:, mid:]
            out.append(full)
        return jnp.concatenate(out, axis=0) + extra

    def exchange_heads(e, attended):
        slots, send, recv = o_slots.at[e], o_send.at[e], o_recv.at[e]
        slots[me] = jnp.concatenate([attended[:half], attended[half:]], axis=1).astype(BF16)
        return send_all(lambda j: slots.at[me], slots, send, recv)

    def gathered_heads(e, copies):
        slots, send, recv = o_slots.at[e], o_send.at[e], o_recv.at[e]
        wait_all(copies, slots, send, recv)
        got = [slots[j].astype(F32) for j in range(n)]
        sides = [jnp.concatenate([g[:, r * head : (r + 1) * head] for g in got], axis=1) for r in range(2)]
        return jnp.concatenate(sides, axis=0).astype(BF16)

    def put_columns(l, k_new, v_new):
        eye = (lax.broadcasted_iota(jnp.int32, (head, head), 0) == lax.broadcasted_iota(jnp.int32, (head, head), 1))
        eye = jnp.where(eye, 1.0, 0.0).astype(BF16)
        wide = batch * LANES
        spread = lax.broadcasted_iota(jnp.int32, (batch, wide), 0) == lax.div(lax.broadcasted_iota(jnp.int32, (batch, wide), 1), LANES)
        spread = jnp.where(spread, 1.0, 0.0).astype(BF16)
        for i, rows in enumerate((k_new, v_new)):
            columns[i] = dot_nn(dot_nt(eye, rows).astype(BF16), spread).astype(BF16)

        def one(b, carry):
            for t in range(0, ctx, LANES):
                size = min(LANES, ctx - t)
                here = jnp.broadcast_to(one_hot[t // LANES, pl.ds(b, 1), :], (head, LANES))[:, :size].astype(BF16) > 0.5
                for i, cache in enumerate((sk, sv)):
                    fresh = columns[i, :, pl.ds(pl.multiple_of(b * LANES, LANES), LANES)][:, :size]
                    cache[l, b, :, t : t + size] = jnp.where(here, fresh, cache[l, b, :, t : t + size])
            return carry

        lax.fori_loop(0, batch, one, 0)

    for l in range(layers):
        ln = ln_layers[l]
        h = layer_norm(x, ln[0, 0:1], ln[0, 1:2])
        if l == 0:
            own[0].wait()
        q = (dot_nt(h, w_qkv[l, 0]) + in_bias[l, 0]).astype(BF16)
        k_new = dot_nt(h, w_qkv[l, 1]).astype(BF16)
        v_new = (dot_nt(h, w_qkv[l, 2]) + in_bias[l, 1]).astype(BF16)
        for c in self_loads[l]:
            c.wait()
        new_score = jnp.sum(q.astype(F32) * k_new.astype(F32), axis=-1, keepdims=True) * (head ** -0.5)

        def finish_self(s):
            s = jnp.where(lax.broadcasted_iota(jnp.int32, s.shape, 1) < place, s, -1e30)
            peak = jnp.maximum(jnp.max(s, axis=-1, keepdims=True), new_score)
            e = jnp.exp(s - peak)
            e_new = jnp.exp(new_score - peak)
            total = jnp.sum(e, axis=-1, keepdims=True) + e_new
            return (e / total).astype(BF16), (e_new / total).astype(BF16).astype(F32) * v_new.astype(F32)

        def finish_cross(s):
            e = jnp.exp(s - jnp.max(s, axis=-1, keepdims=True))
            return (e / jnp.sum(e, axis=-1, keepdims=True)).astype(BF16), 0.0

        attended = attend(q, sk.at[l], sv.at[l], finish_self)
        copies = exchange_heads(2 * l, attended)
        weights_start(2 * l + 1)
        weights_forward(2 * l)
        put_columns(l, k_new, v_new)
        weights_wait(2 * l)
        heads = gathered_heads(2 * l, copies)
        x = x + dot_nn(heads, wo_full[l, 0].reshape(n * head, width)).astype(BF16).astype(F32) + out_bias[0, l : l + 1]

        h = layer_norm(x, ln[1, 0:1], ln[1, 1:2])
        if l == 0:
            for c in own[1:]:
                c.wait()
        q = (dot_nt(h, w_cq[l]) + in_bias[l, 2]).astype(BF16)
        key_loads[l].wait()
        val_loads[l].wait()
        attended = attend(q, ck.at[l], cv, finish_cross)
        copies = exchange_heads(2 * l + 1, attended)
        weights_forward(2 * l + 1)
        weights_wait(2 * l + 1)
        if l + 1 < layers:
            val_loads[l + 1].start()
        heads = gathered_heads(2 * l + 1, copies)
        x = x + dot_nn(heads, wo_full[l, 1].reshape(n * head, width)).astype(BF16).astype(F32) + out_bias[1, l : l + 1]

        h = layer_norm(x, ln[2, 0:1], ln[2, 1:2])
        hidden = dot_nn(h, fc1[l]) + b_fc1[l : l + 1]
        active = (0.5 * hidden * (1.0 + lax.erf(hidden * (0.5 ** 0.5)))).astype(BF16)
        partial = dot_nn(active, fc2[l])
        for j in range(n):
            r, c = j // (n // 2), j % (n // 2)
            rs_src[l, j] = partial[r * half : (r + 1) * half, c * block : (c + 1) * block]
        copies = send_all(lambda j: rs_src.at[l, j], rs_slots.at[l], rs_send.at[l], rs_recv.at[l])
        rs_slots[l, me] = rs_src[l, me]
        if l + 1 < layers:
            weights_start(2 * l + 2)
        wait_all(copies, rs_slots.at[l], rs_send.at[l], rs_recv.at[l])
        total = rs_slots[l, 0]
        for j in range(1, n):
            total = total + rs_slots[l, j]
        ag_slots[l, me] = total.astype(BF16)
        copies = send_all(lambda j: ag_slots.at[l, me], ag_slots.at[l], ag_send.at[l], ag_recv.at[l])
        wait_all(copies, ag_slots.at[l], ag_send.at[l], ag_recv.at[l])
        sides = [jnp.concatenate([ag_slots[l, r * (n // 2) + c].astype(F32) for c in range(n // 2)], axis=1) for r in range(2)]
        x = x + jnp.concatenate(sides, axis=0) + out_bias[2, l : l + 1]

    final_out[...] = layer_norm(x, ln_final[0:1], ln_final[1:2])


def last_kernel(final, table, sk, sv, logits_out, keys_out, vals_out, logits, sems, logit_sems):
    copies = []
    for i, (src, dst) in enumerate(((sk, keys_out), (sv, vals_out))):
        for l in range(sk.shape[0]):
            copies.append(pltpu.make_async_copy(src.at[l], dst.at[l], sems.at[i, l]))
            copies[-1].start()
    h = final[...]
    pieces = logit_sems.shape[0]
    piece = logits.shape[1] // pieces
    for c in range(pieces):
        here = pl.ds(c * piece, piece)
        logits[:, here] = dot_nt(h, table[here, :])
        copies.append(pltpu.make_async_copy(logits.at[:, here], logits_out.at[:, here], logit_sems.at[c]))
        copies[-1].start()
    for c in copies:
        c.wait()


def solution(mesh):
    n = mesh.shape["tp"]

    def local_step(tokens, positions, self_keys, self_vals, cross_keys, cross_vals, embed_table, pos_table, w_qkv, w_cq, in_bias, w_out, out_bias, w_fc1, b_fc1, w_fc2, ln_layers, ln_final):
        layers, batch, ctx, _, head = self_keys.shape
        frames = cross_keys.shape[2]
        shard_rows, width = embed_table.shape
        hidden = w_fc1.shape[2]
        half, block = batch // 2, width // (n // 2)

        def by_place(cache):
            return jnp.transpose(cache[:, :, :, 0, :], (0, 1, 3, 2))

        vmem = pl.BlockSpec(memory_space=pltpu.VMEM)
        hbm = pl.BlockSpec(memory_space=pl.ANY)
        sem = pltpu.SemaphoreType.DMA
        cache_rows = (layers, batch, head, ctx)
        final_hidden, table, sk, sv = pl.pallas_call(
            functools.partial(step_kernel, n),
            out_shape=(pltpu.VMEM((batch, width), BF16), pltpu.VMEM((shard_rows, width), BF16), pltpu.VMEM(cache_rows, BF16), pltpu.VMEM(cache_rows, BF16)),
            in_specs=[vmem] * 7 + [hbm] * 11,
            out_specs=(vmem, vmem, vmem, vmem),
            scratch_shapes=[
                pltpu.VMEM((layers, batch, head, frames), BF16),
                pltpu.VMEM((batch, head, frames), BF16),
                pltpu.VMEM((layers, 2, n, head, width), BF16),
                pltpu.VMEM(pos_table.shape, BF16),
                pltpu.VMEM((layers, 3, head, width), BF16),
                pltpu.VMEM((layers, head, width), BF16),
                pltpu.VMEM(w_fc1.shape, BF16),
                pltpu.VMEM(w_fc2.shape, BF16),
                pltpu.VMEM((batch, width), BF16),
                pltpu.VMEM((batch, width), BF16),
                pltpu.VMEM((2, half, width), BF16),
                pltpu.VMEM((n // 2, 2, half, width), BF16),
                pltpu.VMEM((2 * layers, n, half, 2 * head), BF16),
                pltpu.VMEM((layers, n, half, block), F32),
                pltpu.VMEM((layers, n, half, block), F32),
                pltpu.VMEM((layers, n, half, block), BF16),
                pltpu.VMEM((batch, GROUP * head), BF16),
                pltpu.VMEM((batch, frames), F32),
                pltpu.VMEM((pl.cdiv(ctx, LANES), batch, LANES), F32),
                pltpu.VMEM((2, head, batch * LANES), BF16),
                sem((CHUNKS,)), sem, sem((4,)), sem((layers, 2)), sem((layers, 2)), sem((2 * layers,)),
                sem, sem, sem((n // 2, 2)), sem((n // 2, 2)),
                sem((2 * layers, n)), sem((2 * layers, n)), sem((layers, n)), sem((layers, n)), sem((layers, n)), sem((layers, n)),
                sem((2 * layers, n)), sem((2 * layers, n)),
            ],
            compiler_params=pltpu.CompilerParams(collective_id=0, has_side_effects=True, vmem_limit_bytes=STEP_VMEM),
            name="decode_step",
        )(
            tokens[None], positions[None], in_bias, jnp.transpose(out_bias, (1, 0, 2)), b_fc1, ln_layers, ln_final,
            embed_table, pos_table, jnp.transpose(w_qkv[:, :, :, 0, :], (0, 2, 3, 1)), jnp.transpose(w_cq[:, :, 0, :], (0, 2, 1)),
            w_fc1, w_fc2, w_out[:, :, 0],
            by_place(self_keys), by_place(self_vals), by_place(cross_keys), by_place(cross_vals),
        )

        def in_vmem(a):
            return pltpu.with_memory_space_constraint(a, pltpu.VMEM)

        logits, new_keys, new_vals = pl.pallas_call(
            last_kernel,
            out_shape=(jax.ShapeDtypeStruct((batch, shard_rows), F32), jax.ShapeDtypeStruct(cache_rows, BF16), jax.ShapeDtypeStruct(cache_rows, BF16)),
            in_specs=[vmem] * 4,
            out_specs=(hbm, hbm, hbm),
            scratch_shapes=[pltpu.VMEM((batch, shard_rows), F32), sem((2, layers)), sem((3,))],
            compiler_params=pltpu.CompilerParams(vmem_limit_bytes=LAST_VMEM),
            name="last",
        )(in_vmem(final_hidden), in_vmem(table), in_vmem(sk), in_vmem(sv))

        def as_given(cache):
            return jnp.transpose(cache, (0, 1, 3, 2))[:, :, :, None, :]

        return logits, as_given(new_keys), as_given(new_vals)

    batch_spec = P("dp")
    cache_spec = P(None, "dp", None, "tp", None)
    in_specs = (batch_spec, batch_spec, cache_spec, cache_spec, cache_spec, cache_spec, P("tp", None), P(None, None), P(None, None, None, "tp", None), P(None, None, "tp", None), P(None, None, "tp", None), P(None, None, "tp", None, None), P(None, None, None), P(None, None, "tp"), P(None, "tp"), P(None, "tp", None), P(None, None, None, None), P(None, None))
    out_specs = (P("dp", "tp"), cache_spec, cache_spec)
    return jax.shard_map(local_step, mesh=mesh, in_specs=in_specs, out_specs=out_specs, check_vma=False)
```

```python
import functools

import jax
import jax.numpy as jnp
from jax import lax
from jax.experimental import pallas as pl
from jax.experimental.pallas import tpu as pltpu
from jax.sharding import PartitionSpec as P

MESH = pl.DeviceIdType.MESH
LANES = 128
CHUNKS = 8
STEP_VMEM = 42 * 1024 * 1024
LAST_VMEM = 8 * 1024 * 1024
F32 = jnp.float32
BF16 = jnp.bfloat16
NT = (((1,), (1,)), ((), ()))


def dot_nt(a, b):
    return lax.dot_general(a, b, NT, preferred_element_type=F32)


def dot_nn(a, b):
    return jnp.dot(a, b, preferred_element_type=F32)


def layer_norm(x, gain, shift):
    mean = jnp.mean(x, axis=-1, keepdims=True)
    centred = x - mean
    variance = jnp.mean(centred * centred, axis=-1, keepdims=True)
    return (centred * lax.rsqrt(variance + 1e-5) * gain + shift).astype(BF16)


def step_kernel(
    n, tokens, positions, in_bias, out_bias, b_fc1, ln_layers, ln_final,
    embed, pos_table, w_qkv_hbm, w_cq_hbm, fc1_hbm, fc2_hbm, w_out, self_k, self_v, cross_k, cross_v,
    final_out, table, sk, sv,
    ck, cv, wo_full, pos_vmem, w_qkv, w_cq, fc1, fc2, emb_own, emb_partner, emb_chip, emb_slots, o_slots,
    rs_src, rs_slots, ag_slots, one_hot, columns, x, places, fresh,
    sem_e, sem_p, sem_own, sem_self, sem_cross, sem_w, pair_send, pair_recv, emb_send, emb_recv,
    o_send, o_recv, rs_send, rs_recv, ag_send, ag_recv, w_send, w_recv,
):
    layers, batch = sk.shape[0], sk.shape[1]
    head, ctx = sk.shape[2], sk.shape[3]
    width = table.shape[1]
    half, block = batch // 2, width // (n // 2)
    span = half * head
    me = lax.axis_index("tp")
    core, chip = lax.rem(me, 2), lax.div(me, 2)
    partner = me + 1 - 2 * core

    def peer(k):
        return lax.rem(me + k, n)

    barrier = pltpu.get_barrier_semaphore()
    for k in range(1, n):
        pl.semaphore_signal(barrier, 1, device_id={"tp": peer(k)}, device_id_type=MESH)

    chunks = sem_e.shape[0]
    chunk = table.shape[0] // chunks
    table_loads = [pltpu.make_async_copy(embed.at[pl.ds(c * chunk, chunk)], table.at[pl.ds(c * chunk, chunk)], sem_e.at[c]) for c in range(chunks)]
    for c in table_loads:
        c.start()
    pos_load = pltpu.make_async_copy(pos_table, pos_vmem, sem_p)
    pos_load.start()
    own = [pltpu.make_async_copy(a, b, sem_own.at[i]) for i, (a, b) in enumerate(((w_qkv_hbm, w_qkv), (w_cq_hbm, w_cq), (fc1_hbm, fc1), (fc2_hbm, fc2)))]
    self_loads = [[pltpu.make_async_copy(a.at[l], b.at[l], sem_self.at[l, i]) for i, (a, b) in enumerate(((self_k, sk), (self_v, sv)))] for l in range(layers)]
    key_loads = [pltpu.make_async_copy(cross_k.at[l], ck.at[l], sem_cross.at[l, 0]) for l in range(layers)]
    val_loads = [pltpu.make_async_copy(cross_v.at[l], cv, sem_cross.at[l, 1]) for l in range(layers)]
    later_loads = [own[0], *self_loads[0], *own[1:], key_loads[0], val_loads[0]]

    def remote(src, dst, send, recv, to):
        return pltpu.make_async_remote_copy(src, dst, send, recv, device_id={"tp": to}, device_id_type=MESH)

    order = sorted(range(1, n), key=lambda k: -min(k, n - k))

    def send_all(src_of, slots, send, recv):
        for k in order:
            remote(src_of(peer(k)), slots.at[me], send.at[k], recv.at[me], peer(k)).start()

    def wait_all(slots, send, recv):
        for k in order:
            j = peer(k)
            remote(slots.at[j], slots.at[j], send.at[k], recv.at[j], j).wait_recv()
        for k in order:
            remote(slots.at[me], slots.at[me], send.at[k], recv.at[me], peer(k)).wait_send()

    parts = [(w_out.at[l, a], wo_full.at[l, a]) for l in range(layers) for a in range(2)]
    own_copies, first_hop, second_hop = {}, {}, {}

    def weights_start(i):
        src, full = parts[i]
        own_copies[i] = pltpu.make_async_copy(src, full.at[me], sem_w.at[i])
        own_copies[i].start()
        first_hop[i] = [remote(src, full.at[me], w_send.at[i, k], w_recv.at[i, me], peer(k)) for k in range(2, n, 2)]
        first_hop[i].append(remote(src, full.at[me], w_send.at[i, 1], w_recv.at[i, me], partner))
        for c in first_hop[i]:
            c.start()

    def weights_forward(i):
        src, full = parts[i]
        second_hop[i] = []
        for k in range(2, n, 2):
            j = peer(k)
            remote(src, full.at[j], w_send.at[i, k], w_recv.at[i, j], j).wait_recv()
            c = remote(full.at[j], full.at[j], w_send.at[i, k + 1], w_recv.at[i, j], partner)
            c.start()
            second_hop[i].append(c)

    def weights_wait(i):
        src, full = parts[i]
        remote(src, full.at[partner], w_send.at[i, 1], w_recv.at[i, partner], partner).wait_recv()
        for k in range(2, n, 2):
            j = lax.rem(partner + k, n)
            remote(src, full.at[j], w_send.at[i, k + 1], w_recv.at[i, j], partner).wait_recv()
        for c in first_hop[i] + second_hop[i]:
            c.wait_send()
        own_copies[i].wait()

    def as_column(row):
        i = lax.broadcasted_iota(jnp.int32, (batch, batch), 0)
        j = lax.broadcasted_iota(jnp.int32, (batch, batch), 1)
        return jnp.sum(jnp.where(i == j, jnp.broadcast_to(row.astype(F32), (batch, batch)), 0.0), axis=1, keepdims=True)

    token = as_column(tokens[...]).astype(jnp.int32) - me * table.shape[0]
    place = as_column(positions[...]).astype(jnp.int32)
    pl.semaphore_wait(barrier, n - 1)
    weights_start(0)
    picked = jnp.zeros((batch, width), F32)
    for c in range(chunks):
        table_loads[c].wait()
        hit = lax.broadcasted_iota(jnp.int32, (batch, chunk), 1) + c * chunk == token
        picked = picked + dot_nn(jnp.where(hit, 1.0, 0.0).astype(BF16), table[c * chunk : (c + 1) * chunk])
    for c in later_loads:
        c.start()
    emb_own[...] = picked.astype(BF16)

    pair = remote(emb_own, emb_partner, pair_send, pair_recv, partner)
    pair.start()
    hit = lax.broadcasted_iota(jnp.int32, (batch, ctx), 1) == place
    hit = jnp.where(hit, 1.0, 0.0)
    for t in range(0, ctx, LANES):
        size = min(LANES, ctx - t)
        one_hot[t // LANES, :, :size] = hit[:, t : t + size]
    pos_load.wait()
    pos_rows = dot_nn(hit.astype(BF16), pos_vmem[...])
    pair.wait()
    pair_sum = picked + emb_partner[...].astype(F32)
    for r in range(2):
        emb_chip[r] = pair_sum[r * half : (r + 1) * half].astype(BF16)
    others = [k for k in order]
    sends = []
    for dc in (n // 4, *[d for d in range(1, n // 2) if d != n // 4]):
        for other in range(2):
            to = lax.rem(chip + dc, n // 2) * 2 + lax.rem(core + other, 2)
            sends.append(remote(emb_chip.at[core], emb_slots.at[chip, core], emb_send.at[dc, other], emb_recv.at[chip, core], to))
    for c in sends:
        c.start()
    weights_start(1)
    x_parts = [pair_sum[r * half : (r + 1) * half] for r in range(2)]
    for dc in range(1, n // 2):
        far = lax.rem(chip + dc, n // 2)
        for r in range(2):
            remote(emb_chip.at[0], emb_slots.at[far, r], emb_send.at[dc, r], emb_recv.at[far, r], far * 2 + r).wait_recv()
            x_parts[r] = x_parts[r] + emb_slots[far, r].astype(F32)
    for c in sends:
        c.wait_send()
    for r in range(2):
        x[r] = x_parts[r] + pos_rows[r * half : (r + 1) * half]
        places[r] = jnp.broadcast_to(place[r * half : (r + 1) * half], (half, LANES))

    diagonal = lax.broadcasted_iota(jnp.int32, (half, span), 0) == lax.div(lax.broadcasted_iota(jnp.int32, (half, span), 1), head)

    def attend(q, keys, vals, finish):
        length = keys.shape[2]
        wide = jnp.where(diagonal, jnp.concatenate([q] * half, axis=1), 0).astype(BF16)
        scores = dot_nn(wide, keys[...].reshape(span, length))
        weights, extra = finish(scores * (head ** -0.5))
        full = jnp.where(diagonal, dot_nt(weights, vals[...].reshape(span, length)), 0.0)
        total = full[:, :LANES]
        for c in range(LANES, span, LANES):
            total = total + full[:, c : c + LANES]
        out = total[:, :head]
        for c in range(head, LANES, head):
            out = out + total[:, c : c + head]
        return out + extra

    def head_slots(e, r):
        return o_slots.at[e, r], o_send.at[e, r], o_recv.at[e, r]

    def exchange_heads(e, r, attended):
        slots, send, recv = head_slots(e, r)
        slots[me] = attended.astype(BF16)
        send_all(lambda j: slots.at[me], slots, send, recv)

    def gathered_heads(e, r):
        slots, send, recv = head_slots(e, r)
        wait_all(slots, send, recv)
        return jnp.concatenate([slots[j].astype(F32) for j in range(n)], axis=1).astype(BF16)

    def project(l, a, heads):
        return dot_nn(heads, wo_full[l, a].reshape(n * head, width)).astype(BF16).astype(F32)

    def put_columns(l):
        eye = (lax.broadcasted_iota(jnp.int32, (head, head), 0) == lax.broadcasted_iota(jnp.int32, (head, head), 1))
        eye = jnp.where(eye, 1.0, 0.0).astype(BF16)
        wide = batch * LANES
        spread = lax.broadcasted_iota(jnp.int32, (batch, wide), 0) == lax.div(lax.broadcasted_iota(jnp.int32, (batch, wide), 1), LANES)
        spread = jnp.where(spread, 1.0, 0.0).astype(BF16)
        for i in range(2):
            rows = jnp.concatenate([fresh[i, 0], fresh[i, 1]], axis=0).astype(BF16)
            columns[i] = dot_nn(dot_nt(eye, rows).astype(BF16), spread).astype(BF16)

        def one(b, carry):
            for t in range(0, ctx, LANES):
                size = min(LANES, ctx - t)
                here = jnp.broadcast_to(one_hot[t // LANES, pl.ds(b, 1), :], (head, LANES))[:, :size].astype(BF16) > 0.5
                for i, cache in enumerate((sk, sv)):
                    fresh = columns[i, :, pl.ds(pl.multiple_of(b * LANES, LANES), LANES)][:, :size]
                    cache[l, b, :, t : t + size] = jnp.where(here, fresh, cache[l, b, :, t : t + size])
            return carry

        lax.fori_loop(0, batch, one, 0)

    def self_stage(l, r):
        ln = ln_layers[l]
        rows = pl.ds(r * half, half)
        h = layer_norm(x[r], ln[0, 0:1], ln[0, 1:2])
        q = (dot_nt(h, w_qkv[l, 0]) + in_bias[l, 0]).astype(BF16)
        k_new = dot_nt(h, w_qkv[l, 1]).astype(BF16)
        v_new = (dot_nt(h, w_qkv[l, 2]) + in_bias[l, 1]).astype(BF16)
        fresh[0, r] = k_new.astype(F32)
        fresh[1, r] = v_new.astype(F32)
        here = places[r][:, :1]
        new_score = jnp.sum(q.astype(F32) * k_new.astype(F32), axis=-1, keepdims=True) * (head ** -0.5)

        def finish(s):
            s = jnp.where(lax.broadcasted_iota(jnp.int32, s.shape, 1) < here, s, -1e30)
            peak = jnp.maximum(jnp.max(s, axis=-1, keepdims=True), new_score)
            e = jnp.exp(s - peak)
            e_new = jnp.exp(new_score - peak)
            total = jnp.sum(e, axis=-1, keepdims=True) + e_new
            return (e / total).astype(BF16), (e_new / total).astype(BF16).astype(F32) * v_new.astype(F32)

        attended = attend(q, sk.at[l, rows], sv.at[l, rows], finish)
        exchange_heads(2 * l, r, attended)

    def cross_stage(l, r):
        ln = ln_layers[l]
        rows = pl.ds(r * half, half)
        x[r] = x[r] + project(l, 0, gathered_heads(2 * l, r)) + out_bias[0, l : l + 1]
        h = layer_norm(x[r], ln[1, 0:1], ln[1, 1:2])
        q = (dot_nt(h, w_cq[l]) + in_bias[l, 2]).astype(BF16)

        def finish(s):
            e = jnp.exp(s - jnp.max(s, axis=-1, keepdims=True))
            return (e / jnp.sum(e, axis=-1, keepdims=True)).astype(BF16), 0.0

        attended = attend(q, ck.at[l, rows], cv.at[rows], finish)
        exchange_heads(2 * l + 1, r, attended)

    def mlp_stage(l, r):
        ln = ln_layers[l]
        x[r] = x[r] + project(l, 1, gathered_heads(2 * l + 1, r)) + out_bias[1, l : l + 1]
        h = layer_norm(x[r], ln[2, 0:1], ln[2, 1:2])
        hidden = dot_nn(h, fc1[l]) + b_fc1[l : l + 1]
        active = (0.5 * hidden * (1.0 + lax.erf(hidden * (0.5 ** 0.5)))).astype(BF16)
        partial = dot_nn(active, fc2[l])
        for c in range(n // 2):
            rs_src[l, r * (n // 2) + c] = partial[:, c * block : (c + 1) * block]
        for k in order:
            pl.when(lax.div(peer(k), n // 2) == r)(rs_copy(l, k).start)

    def rs_copy(l, k):
        j = peer(k)
        return remote(rs_src.at[l, j], rs_slots.at[l, me], rs_send.at[l, k], rs_recv.at[l, me], j)

    def sum_stage(l):
        wait_all(rs_slots.at[l], rs_send.at[l], rs_recv.at[l])
        rs_slots[l, me] = rs_src[l, me]
        total = rs_slots[l, 0]
        for j in range(1, n):
            total = total + rs_slots[l, j]
        ag_slots[l, me] = total.astype(BF16)
        send_all(lambda j: ag_slots.at[l, me], ag_slots.at[l], ag_send.at[l], ag_recv.at[l])

    def add_stage(l, r):
        for k in order:
            j = peer(k)
            slot = ag_slots.at[l, j]
            pl.when(lax.div(j, n // 2) == r)(remote(slot, slot, ag_send.at[l, k], ag_recv.at[l, j], j).wait_recv)
        x[r] = x[r] + jnp.concatenate([ag_slots[l, r * (n // 2) + c].astype(F32) for c in range(n // 2)], axis=1) + out_bias[2, l : l + 1]

    def both(stage, l):
        def one(r, carry):
            stage(l, r)
            return carry

        lax.fori_loop(0, 2, one, 0)

    def sent(l):
        for k in order:
            remote(ag_slots.at[l, me], ag_slots.at[l, me], ag_send.at[l, k], ag_recv.at[l, me], peer(k)).wait_send()

    def next_stage(l, r):
        add_stage(l - 1, r)
        self_stage(l, r)

    def end_stage(l, r):
        add_stage(l - 1, r)
        final_out[pl.ds(pl.multiple_of(r * half, half), half)] = layer_norm(x[r], ln_final[0:1], ln_final[1:2])

    own[0].wait()
    for c in self_loads[0]:
        c.wait()
    both(self_stage, 0)
    for l in range(layers):
        last = l + 1 == layers
        weights_forward(2 * l)
        if l == 0:
            for c in own[1:]:
                c.wait()
        weights_wait(2 * l)
        key_loads[l].wait()
        val_loads[l].wait()
        if not last:
            for c in (*self_loads[l + 1], key_loads[l + 1]):
                c.start()
        both(cross_stage, l)
        if not last:
            val_loads[l + 1].start()
            weights_start(2 * l + 2)
        weights_forward(2 * l + 1)
        weights_wait(2 * l + 1)
        both(mlp_stage, l)
        if not last:
            weights_start(2 * l + 3)
        put_columns(l)
        sum_stage(l)
        if not last:
            for c in self_loads[l + 1]:
                c.wait()
            both(next_stage, l + 1)
        else:
            both(end_stage, l + 1)
        sent(l)


def last_kernel(final, table, sk, sv, logits_out, keys_out, vals_out, logits, sems, logit_sems):
    copies = []
    for i, (src, dst) in enumerate(((sk, keys_out), (sv, vals_out))):
        for l in range(sk.shape[0]):
            copies.append(pltpu.make_async_copy(src.at[l], dst.at[l], sems.at[i, l]))
            copies[-1].start()
    h = final[...]
    pieces = logit_sems.shape[0]
    piece = logits.shape[1] // pieces
    for c in range(pieces):
        here = pl.ds(c * piece, piece)
        logits[:, here] = dot_nt(h, table[here, :])
        copies.append(pltpu.make_async_copy(logits.at[:, here], logits_out.at[:, here], logit_sems.at[c]))
        copies[-1].start()
    for c in copies:
        c.wait()


def solution(mesh):
    n = mesh.shape["tp"]

    def local_step(tokens, positions, self_keys, self_vals, cross_keys, cross_vals, embed_table, pos_table, w_qkv, w_cq, in_bias, w_out, out_bias, w_fc1, b_fc1, w_fc2, ln_layers, ln_final):
        layers, batch, ctx, _, head = self_keys.shape
        frames = cross_keys.shape[2]
        shard_rows, width = embed_table.shape
        hidden = w_fc1.shape[2]
        half, block = batch // 2, width // (n // 2)

        def by_place(cache):
            return jnp.transpose(cache[:, :, :, 0, :], (0, 1, 3, 2))

        vmem = pl.BlockSpec(memory_space=pltpu.VMEM)
        hbm = pl.BlockSpec(memory_space=pl.ANY)
        sem = pltpu.SemaphoreType.DMA
        cache_rows = (layers, batch, head, ctx)
        final_hidden, table, sk, sv = pl.pallas_call(
            functools.partial(step_kernel, n),
            out_shape=(pltpu.VMEM((batch, width), BF16), pltpu.VMEM((shard_rows, width), BF16), pltpu.VMEM(cache_rows, BF16), pltpu.VMEM(cache_rows, BF16)),
            in_specs=[vmem] * 7 + [hbm] * 11,
            out_specs=(vmem, vmem, vmem, vmem),
            scratch_shapes=[
                pltpu.VMEM((layers, batch, head, frames), BF16),
                pltpu.VMEM((batch, head, frames), BF16),
                pltpu.VMEM((layers, 2, n, head, width), BF16),
                pltpu.VMEM(pos_table.shape, BF16),
                pltpu.VMEM((layers, 3, head, width), BF16),
                pltpu.VMEM((layers, head, width), BF16),
                pltpu.VMEM(w_fc1.shape, BF16),
                pltpu.VMEM(w_fc2.shape, BF16),
                pltpu.VMEM((batch, width), BF16),
                pltpu.VMEM((batch, width), BF16),
                pltpu.VMEM((2, half, width), BF16),
                pltpu.VMEM((n // 2, 2, half, width), BF16),
                pltpu.VMEM((2 * layers, 2, n, half, head), BF16),
                pltpu.VMEM((layers, n, half, block), F32),
                pltpu.VMEM((layers, n, half, block), F32),
                pltpu.VMEM((layers, n, half, block), BF16),
                pltpu.VMEM((pl.cdiv(ctx, LANES), batch, LANES), F32),
                pltpu.VMEM((2, head, batch * LANES), BF16),
                pltpu.VMEM((2, half, width), F32),
                pltpu.VMEM((2, half, LANES), jnp.int32),
                pltpu.VMEM((2, 2, half, head), F32),
                sem((CHUNKS,)), sem, sem((4,)), sem((layers, 2)), sem((layers, 2)), sem((2 * layers,)),
                sem, sem, sem((n // 2, 2)), sem((n // 2, 2)),
                sem((2 * layers, 2, n)), sem((2 * layers, 2, n)), sem((layers, n)), sem((layers, n)), sem((layers, n)), sem((layers, n)),
                sem((2 * layers, n)), sem((2 * layers, n)),
            ],
            compiler_params=pltpu.CompilerParams(collective_id=0, has_side_effects=True, vmem_limit_bytes=STEP_VMEM),
            name="decode_step",
        )(
            tokens[None], positions[None], in_bias, jnp.transpose(out_bias, (1, 0, 2)), b_fc1, ln_layers, ln_final,
            embed_table, pos_table, jnp.transpose(w_qkv[:, :, :, 0, :], (0, 2, 3, 1)), jnp.transpose(w_cq[:, :, 0, :], (0, 2, 1)),
            w_fc1, w_fc2, w_out[:, :, 0],
            by_place(self_keys), by_place(self_vals), by_place(cross_keys), by_place(cross_vals),
        )

        def in_vmem(a):
            return pltpu.with_memory_space_constraint(a, pltpu.VMEM)

        logits, new_keys, new_vals = pl.pallas_call(
            last_kernel,
            out_shape=(jax.ShapeDtypeStruct((batch, shard_rows), F32), jax.ShapeDtypeStruct(cache_rows, BF16), jax.ShapeDtypeStruct(cache_rows, BF16)),
            in_specs=[vmem] * 4,
            out_specs=(hbm, hbm, hbm),
            scratch_shapes=[pltpu.VMEM((batch, shard_rows), F32), sem((2, layers)), sem((3,))],
            compiler_params=pltpu.CompilerParams(vmem_limit_bytes=LAST_VMEM),
            name="last",
        )(in_vmem(final_hidden), in_vmem(table), in_vmem(sk), in_vmem(sv))

        def as_given(cache):
            return jnp.transpose(cache, (0, 1, 3, 2))[:, :, :, None, :]

        return logits, as_given(new_keys), as_given(new_vals)

    batch_spec = P("dp")
    cache_spec = P(None, "dp", None, "tp", None)
    in_specs = (batch_spec, batch_spec, cache_spec, cache_spec, cache_spec, cache_spec, P("tp", None), P(None, None), P(None, None, None, "tp", None), P(None, None, "tp", None), P(None, None, "tp", None), P(None, None, "tp", None, None), P(None, None, None), P(None, None, "tp"), P(None, "tp"), P(None, "tp", None), P(None, None, None, None), P(None, None))
    out_specs = (P("dp", "tp"), cache_spec, cache_spec)
    return jax.shard_map(local_step, mesh=mesh, in_specs=in_specs, out_specs=out_specs, check_vma=False)
```

```python
import functools

import jax
import jax.numpy as jnp
from jax import lax
from jax.experimental import pallas as pl
from jax.experimental.pallas import tpu as pltpu
from jax.sharding import PartitionSpec as P

MESH = pl.DeviceIdType.MESH
LANES = 128
GROUP = 8
CHUNKS = 8
SMALL = 7
STEP_VMEM = 42 * 1024 * 1024
LAST_VMEM = 8 * 1024 * 1024
F32 = jnp.float32
BF16 = jnp.bfloat16
NT = (((1,), (1,)), ((), ()))


def dot_nt(a, b):
    return lax.dot_general(a, b, NT, preferred_element_type=F32)


def dot_nn(a, b):
    return jnp.dot(a, b, preferred_element_type=F32)


def layer_norm(x, gain, shift):
    mean = jnp.mean(x, axis=-1, keepdims=True)
    centred = x - mean
    variance = jnp.mean(centred * centred, axis=-1, keepdims=True)
    return (centred * lax.rsqrt(variance + 1e-5) * gain + shift).astype(BF16)


def step_kernel(
    n, *refs,
):
    small_hbm, refs = refs[:SMALL], refs[SMALL:]
    (
    embed, pos_table, w_qkv_hbm, w_cq_hbm, fc1_hbm, fc2_hbm, w_out, self_k, self_v, cross_k, cross_v,
    final_out, table, sk, sv,
    ck, cv, wo_full, pos_vmem, w_qkv, w_cq, fc1, fc2, emb_own, emb_partner, emb_chip, emb_slots, o_slots,
    rs_src, rs_slots, ag_slots, one_hot, columns, x, places, fresh,
    sem_e, sem_p, sem_own, sem_self, sem_cross, sem_w, pair_send, pair_recv, emb_send, emb_recv,
    o_send, o_recv, rs_send, rs_recv, ag_send, ag_recv, w_send, w_recv,
    small, sem_small,
    ) = (*refs[:-SMALL - 1], refs[-SMALL - 1 : -1], refs[-1])
    tokens, positions, in_bias, out_bias, b_fc1, ln_layers, ln_final = small
    small_loads = [pltpu.make_async_copy(a, b, sem_small.at[i]) for i, (a, b) in enumerate(zip(small_hbm, small))]
    for c in small_loads:
        c.start()
    layers, batch = sk.shape[0], sk.shape[1]
    head, ctx = sk.shape[2], sk.shape[3]
    width = table.shape[1]
    half, block = batch // 2, width // (n // 2)
    me = lax.axis_index("tp")
    core, chip = lax.rem(me, 2), lax.div(me, 2)
    partner = me + 1 - 2 * core

    def peer(k):
        return lax.rem(me + k, n)

    barrier = pltpu.get_barrier_semaphore()
    for k in range(1, n):
        pl.semaphore_signal(barrier, 1, device_id={"tp": peer(k)}, device_id_type=MESH)

    chunks = sem_e.shape[0]
    chunk = table.shape[0] // chunks
    table_loads = [pltpu.make_async_copy(embed.at[pl.ds(c * chunk, chunk)], table.at[pl.ds(c * chunk, chunk)], sem_e.at[c]) for c in range(chunks)]
    for c in table_loads:
        c.start()
    pos_load = pltpu.make_async_copy(pos_table, pos_vmem, sem_p)
    pos_load.start()
    own = [pltpu.make_async_copy(a, b, sem_own.at[i]) for i, (a, b) in enumerate(((w_qkv_hbm, w_qkv), (w_cq_hbm, w_cq), (fc1_hbm, fc1), (fc2_hbm, fc2)))]
    self_loads = [[pltpu.make_async_copy(a.at[l], b.at[l], sem_self.at[l, i]) for i, (a, b) in enumerate(((self_k, sk), (self_v, sv)))] for l in range(layers)]
    key_loads = [pltpu.make_async_copy(cross_k.at[l], ck.at[l], sem_cross.at[l, 0]) for l in range(layers)]
    val_loads = [pltpu.make_async_copy(cross_v.at[l], cv, sem_cross.at[l, 1]) for l in range(layers)]
    later_loads = [own[0], *self_loads[0], *own[1:], key_loads[0], val_loads[0]]

    def remote(src, dst, send, recv, to):
        return pltpu.make_async_remote_copy(src, dst, send, recv, device_id={"tp": to}, device_id_type=MESH)

    order = sorted(range(1, n), key=lambda k: -min(k, n - k))

    def send_all(src_of, slots, send, recv):
        for k in order:
            remote(src_of(peer(k)), slots.at[me], send.at[k], recv.at[me], peer(k)).start()

    def wait_all(slots, send, recv):
        for k in order:
            j = peer(k)
            remote(slots.at[j], slots.at[j], send.at[k], recv.at[j], j).wait_recv()
        for k in order:
            remote(slots.at[me], slots.at[me], send.at[k], recv.at[me], peer(k)).wait_send()

    parts = [(w_out.at[l, a], wo_full.at[l, a]) for l in range(layers) for a in range(2)]
    own_copies, first_hop, second_hop = {}, {}, {}

    def weights_start(i):
        src, full = parts[i]
        own_copies[i] = pltpu.make_async_copy(src, full.at[me], sem_w.at[i])
        own_copies[i].start()
        first_hop[i] = [remote(src, full.at[me], w_send.at[i, k], w_recv.at[i, me], peer(k)) for k in range(2, n, 2)]
        first_hop[i].append(remote(src, full.at[me], w_send.at[i, 1], w_recv.at[i, me], partner))
        for c in first_hop[i]:
            c.start()

    def weights_forward(i):
        src, full = parts[i]
        second_hop[i] = []
        for k in range(2, n, 2):
            j = peer(k)
            remote(src, full.at[j], w_send.at[i, k], w_recv.at[i, j], j).wait_recv()
            c = remote(full.at[j], full.at[j], w_send.at[i, k + 1], w_recv.at[i, j], partner)
            c.start()
            second_hop[i].append(c)

    def weights_wait(i):
        src, full = parts[i]
        remote(src, full.at[partner], w_send.at[i, 1], w_recv.at[i, partner], partner).wait_recv()
        for k in range(2, n, 2):
            j = lax.rem(partner + k, n)
            remote(src, full.at[j], w_send.at[i, k + 1], w_recv.at[i, j], partner).wait_recv()
        for c in first_hop[i] + second_hop[i]:
            c.wait_send()
        own_copies[i].wait()

    def as_column(row):
        i = lax.broadcasted_iota(jnp.int32, (batch, batch), 0)
        j = lax.broadcasted_iota(jnp.int32, (batch, batch), 1)
        return jnp.sum(jnp.where(i == j, jnp.broadcast_to(row.astype(F32), (batch, batch)), 0.0), axis=1, keepdims=True)

    for c in small_loads:
        c.wait()
    token = as_column(tokens[...]).astype(jnp.int32) - me * table.shape[0]
    place = as_column(positions[...]).astype(jnp.int32)
    pl.semaphore_wait(barrier, n - 1)
    weights_start(0)
    picked = jnp.zeros((batch, width), F32)
    for c in range(chunks):
        table_loads[c].wait()
        hit = lax.broadcasted_iota(jnp.int32, (batch, chunk), 1) + c * chunk == token
        picked = picked + dot_nn(jnp.where(hit, 1.0, 0.0).astype(BF16), table[c * chunk : (c + 1) * chunk])
    for c in later_loads:
        c.start()
    emb_own[...] = picked.astype(BF16)

    pair = remote(emb_own, emb_partner, pair_send, pair_recv, partner)
    pair.start()
    hit = lax.broadcasted_iota(jnp.int32, (batch, ctx), 1) == place
    hit = jnp.where(hit, 1.0, 0.0)
    for t in range(0, ctx, LANES):
        size = min(LANES, ctx - t)
        one_hot[t // LANES, :, :size] = hit[:, t : t + size]
    pos_load.wait()
    pos_rows = dot_nn(hit.astype(BF16), pos_vmem[...])
    pair.wait()
    pair_sum = picked + emb_partner[...].astype(F32)
    for r in range(2):
        emb_chip[r] = pair_sum[r * half : (r + 1) * half].astype(BF16)
    cols = width // 2
    distances = (n // 4, *[d for d in range(1, n // 2) if d != n // 4])

    def table_hop(dc, other, r):
        to = lax.rem(chip + dc, n // 2) * 2 + lax.rem(core + other, 2)
        here = pl.ds(pl.multiple_of(core * cols, LANES), cols)
        return remote(emb_chip.at[r, :, here], emb_slots.at[chip, r, :, here], emb_send.at[r, dc, other], emb_recv.at[r, chip, core], to)

    for r in range(2):
        for dc in distances:
            for other in range(2):
                table_hop(dc, other, r).start()
    weights_start(1)
    for r in range(2):
        x[r] = pair_sum[r * half : (r + 1) * half] + pos_rows[r * half : (r + 1) * half]
        places[r] = jnp.broadcast_to(place[r * half : (r + 1) * half], (half, LANES))

    def table_stage(r):
        total = x[r]
        for dc in reversed(distances):
            far = lax.rem(chip + dc, n // 2)
            for c in range(2):
                slot = emb_slots.at[far, r, :, c * cols : (c + 1) * cols]
                remote(slot, slot, emb_send.at[r, dc, c], emb_recv.at[r, far, c], far * 2 + c).wait_recv()
            total = total + emb_slots[far, r].astype(F32)
        x[r] = total

    def table_sent():
        for r in range(2):
            for dc in distances:
                for other in range(2):
                    table_hop(dc, other, r).wait_send()

    span = GROUP * head
    diagonal = lax.broadcasted_iota(jnp.int32, (GROUP, span), 0) == lax.div(lax.broadcasted_iota(jnp.int32, (GROUP, span), 1), head)

    def attend(q, keys, vals, finish):
        length = keys.shape[2]
        q = q.astype(F32)
        groups = [slice(g, g + GROUP) for g in range(0, half, GROUP)]
        wide = [jnp.where(diagonal, jnp.concatenate([q[rows]] * GROUP, axis=1), 0.0).astype(BF16) for rows in groups]
        scores = [dot_nn(w, keys[rows].reshape(span, length)) for w, rows in zip(wide, groups)]
        finished = [finish(s * (head ** -0.5), rows) for s, rows in zip(scores, groups)]
        out = []
        for (weights, extra), rows in zip(finished, groups):
            full = jnp.where(diagonal, dot_nt(weights, vals[rows].reshape(span, length)), 0.0)
            total = full[:, :LANES]
            for c in range(LANES, span, LANES):
                total = total + full[:, c : c + LANES]
            mixed = total[:, :head]
            for c in range(head, LANES, head):
                mixed = mixed + total[:, c : c + head]
            out.append(mixed + extra)
        return jnp.concatenate(out, axis=0)

    def head_slots(e, r):
        return o_slots.at[e, r], o_send.at[e, r], o_recv.at[e, r]

    def exchange_heads(e, r, attended):
        slots, send, recv = head_slots(e, r)
        slots[me] = attended.astype(BF16)
        send_all(lambda j: slots.at[me], slots, send, recv)

    def project(l, a, r):
        slots, send, recv = head_slots(2 * l + a, r)
        total = dot_nn(slots[me], wo_full[l, a, me])
        for k in reversed(order):
            j = peer(k)
            remote(slots.at[j], slots.at[j], send.at[k], recv.at[j], j).wait_recv()
            total = total + dot_nn(slots[j], wo_full[l, a, j])
        for k in order:
            remote(slots.at[me], slots.at[me], send.at[k], recv.at[me], peer(k)).wait_send()
        return total.astype(BF16).astype(F32)

    def put_columns(l):
        eye = (lax.broadcasted_iota(jnp.int32, (head, head), 0) == lax.broadcasted_iota(jnp.int32, (head, head), 1))
        eye = jnp.where(eye, 1.0, 0.0).astype(BF16)
        wide = batch * LANES
        spread = lax.broadcasted_iota(jnp.int32, (batch, wide), 0) == lax.div(lax.broadcasted_iota(jnp.int32, (batch, wide), 1), LANES)
        spread = jnp.where(spread, 1.0, 0.0).astype(BF16)
        for i in range(2):
            rows = jnp.concatenate([fresh[i, 0], fresh[i, 1]], axis=0).astype(BF16)
            columns[i] = dot_nn(dot_nt(eye, rows).astype(BF16), spread).astype(BF16)

        def one(b, carry):
            for t in range(0, ctx, LANES):
                size = min(LANES, ctx - t)
                here = jnp.broadcast_to(one_hot[t // LANES, pl.ds(b, 1), :], (head, LANES))[:, :size].astype(BF16) > 0.5
                for i, cache in enumerate((sk, sv)):
                    fresh = columns[i, :, pl.ds(pl.multiple_of(b * LANES, LANES), LANES)][:, :size]
                    cache[l, b, :, t : t + size] = jnp.where(here, fresh, cache[l, b, :, t : t + size])
            return carry

        lax.fori_loop(0, batch, one, 0)

    def self_stage(l, r):
        ln = ln_layers[l]
        rows = pl.ds(r * half, half)
        h = layer_norm(x[r], ln[0, 0:1], ln[0, 1:2])
        q = (dot_nt(h, w_qkv[l, 0]) + in_bias[l, 0]).astype(BF16)
        k_new = dot_nt(h, w_qkv[l, 1]).astype(BF16)
        v_new = (dot_nt(h, w_qkv[l, 2]) + in_bias[l, 1]).astype(BF16)
        fresh[0, r] = k_new.astype(F32)
        fresh[1, r] = v_new.astype(F32)
        here = places[r][:, :1]
        all_new = jnp.sum(q.astype(F32) * k_new.astype(F32), axis=-1, keepdims=True) * (head ** -0.5)

        def finish(s, rows):
            new_score = all_new[rows]
            s = jnp.where(lax.broadcasted_iota(jnp.int32, s.shape, 1) < here[rows], s, -1e30)
            peak = jnp.maximum(jnp.max(s, axis=-1, keepdims=True), new_score)
            e = jnp.exp(s - peak)
            e_new = jnp.exp(new_score - peak)
            total = jnp.sum(e, axis=-1, keepdims=True) + e_new
            return (e / total).astype(BF16), (e_new / total).astype(BF16).astype(F32) * v_new.astype(F32)[rows]

        attended = attend(q, sk.at[l, rows], sv.at[l, rows], finish)
        exchange_heads(2 * l, r, attended)

    def cross_stage(l, r):
        ln = ln_layers[l]
        rows = pl.ds(r * half, half)
        x[r] = x[r] + project(l, 0, r) + out_bias[0, l : l + 1]
        h = layer_norm(x[r], ln[1, 0:1], ln[1, 1:2])
        q = (dot_nt(h, w_cq[l]) + in_bias[l, 2]).astype(BF16)

        def finish(s, rows):
            e = jnp.exp(s - jnp.max(s, axis=-1, keepdims=True))
            return (e / jnp.sum(e, axis=-1, keepdims=True)).astype(BF16), 0.0

        attended = attend(q, ck.at[l, rows], cv.at[rows], finish)
        exchange_heads(2 * l + 1, r, attended)

    def mlp_stage(l, r):
        ln = ln_layers[l]
        x[r] = x[r] + project(l, 1, r) + out_bias[1, l : l + 1]
        h = layer_norm(x[r], ln[2, 0:1], ln[2, 1:2])
        hidden = dot_nn(h, fc1[l]) + b_fc1[l : l + 1]
        active = (0.5 * hidden * (1.0 + lax.erf(hidden * (0.5 ** 0.5)))).astype(BF16)
        partial = dot_nn(active, fc2[l])
        for c in range(n // 2):
            rs_src[l, r * (n // 2) + c] = partial[:, c * block : (c + 1) * block]
        for k in order:
            pl.when(lax.div(peer(k), n // 2) == r)(rs_copy(l, k).start)

    def rs_copy(l, k):
        j = peer(k)
        return remote(rs_src.at[l, j], rs_slots.at[l, me], rs_send.at[l, k], rs_recv.at[l, me], j)

    def sum_stage(l):
        wait_all(rs_slots.at[l], rs_send.at[l], rs_recv.at[l])
        rs_slots[l, me] = rs_src[l, me]
        total = rs_slots[l, 0]
        for j in range(1, n):
            total = total + rs_slots[l, j]
        ag_slots[l, me] = total.astype(BF16)
        send_all(lambda j: ag_slots.at[l, me], ag_slots.at[l], ag_send.at[l], ag_recv.at[l])

    def add_stage(l, r):
        for k in order:
            j = peer(k)
            slot = ag_slots.at[l, j]
            pl.when(lax.div(j, n // 2) == r)(remote(slot, slot, ag_send.at[l, k], ag_recv.at[l, j], j).wait_recv)
        x[r] = x[r] + jnp.concatenate([ag_slots[l, r * (n // 2) + c].astype(F32) for c in range(n // 2)], axis=1) + out_bias[2, l : l + 1]

    def both(stage, l):
        def one(r, carry):
            stage(l, r)
            return carry

        lax.fori_loop(0, 2, one, 0)

    def sent(l):
        for k in order:
            remote(ag_slots.at[l, me], ag_slots.at[l, me], ag_send.at[l, k], ag_recv.at[l, me], peer(k)).wait_send()

    def first_stage(l, r):
        table_stage(r)
        self_stage(l, r)

    def next_stage(l, r):
        add_stage(l - 1, r)
        self_stage(l, r)

    def end_stage(l, r):
        add_stage(l - 1, r)
        final_out[pl.ds(pl.multiple_of(r * half, half), half)] = layer_norm(x[r], ln_final[0:1], ln_final[1:2])

    own[0].wait()
    for c in self_loads[0]:
        c.wait()
    both(first_stage, 0)
    table_sent()
    for l in range(layers):
        last = l + 1 == layers
        weights_forward(2 * l)
        if l == 0:
            for c in own[1:]:
                c.wait()
        weights_wait(2 * l)
        key_loads[l].wait()
        val_loads[l].wait()
        if not last:
            for c in (*self_loads[l + 1], key_loads[l + 1]):
                c.start()
        both(cross_stage, l)
        if not last:
            val_loads[l + 1].start()
            weights_start(2 * l + 2)
        weights_forward(2 * l + 1)
        weights_wait(2 * l + 1)
        both(mlp_stage, l)
        if not last:
            weights_start(2 * l + 3)
        put_columns(l)
        sum_stage(l)
        if not last:
            for c in self_loads[l + 1]:
                c.wait()
            both(next_stage, l + 1)
        else:
            both(end_stage, l + 1)
        sent(l)


def last_kernel(final, table, sk, sv, logits_out, keys_out, vals_out, logits, sems, logit_sems):
    copies = []
    for i, (src, dst) in enumerate(((sk, keys_out), (sv, vals_out))):
        for l in range(sk.shape[0]):
            copies.append(pltpu.make_async_copy(src.at[l], dst.at[l], sems.at[i, l]))
            copies[-1].start()
    h = final[...]
    pieces = logit_sems.shape[0]
    piece = logits.shape[1] // pieces
    for c in range(pieces):
        here = pl.ds(c * piece, piece)
        logits[:, here] = dot_nt(h, table[here, :])
        copies.append(pltpu.make_async_copy(logits.at[:, here], logits_out.at[:, here], logit_sems.at[c]))
        copies[-1].start()
    for c in copies:
        c.wait()


def solution(mesh):
    n = mesh.shape["tp"]

    def local_step(tokens, positions, self_keys, self_vals, cross_keys, cross_vals, embed_table, pos_table, w_qkv, w_cq, in_bias, w_out, out_bias, w_fc1, b_fc1, w_fc2, ln_layers, ln_final):
        layers, batch, ctx, _, head = self_keys.shape
        frames = cross_keys.shape[2]
        shard_rows, width = embed_table.shape
        hidden = w_fc1.shape[2]
        half, block = batch // 2, width // (n // 2)

        def by_place(cache):
            return jnp.transpose(cache[:, :, :, 0, :], (0, 1, 3, 2))

        vmem = pl.BlockSpec(memory_space=pltpu.VMEM)
        hbm = pl.BlockSpec(memory_space=pl.ANY)
        sem = pltpu.SemaphoreType.DMA
        cache_rows = (layers, batch, head, ctx)
        small = (tokens[None], positions[None], in_bias, jnp.transpose(out_bias, (1, 0, 2)), b_fc1, ln_layers, ln_final)
        final_hidden, table, sk, sv = pl.pallas_call(
            functools.partial(step_kernel, n),
            out_shape=(pltpu.VMEM((batch, width), BF16), pltpu.VMEM((shard_rows, width), BF16), pltpu.VMEM(cache_rows, BF16), pltpu.VMEM(cache_rows, BF16)),
            in_specs=[hbm] * (SMALL + 11),
            out_specs=(vmem, vmem, vmem, vmem),
            scratch_shapes=[
                pltpu.VMEM((layers, batch, head, frames), BF16),
                pltpu.VMEM((batch, head, frames), BF16),
                pltpu.VMEM((layers, 2, n, head, width), BF16),
                pltpu.VMEM(pos_table.shape, BF16),
                pltpu.VMEM((layers, 3, head, width), BF16),
                pltpu.VMEM((layers, head, width), BF16),
                pltpu.VMEM(w_fc1.shape, BF16),
                pltpu.VMEM(w_fc2.shape, BF16),
                pltpu.VMEM((batch, width), BF16),
                pltpu.VMEM((batch, width), BF16),
                pltpu.VMEM((2, half, width), BF16),
                pltpu.VMEM((n // 2, 2, half, width), BF16),
                pltpu.VMEM((2 * layers, 2, n, half, head), BF16),
                pltpu.VMEM((layers, n, half, block), F32),
                pltpu.VMEM((layers, n, half, block), F32),
                pltpu.VMEM((layers, n, half, block), BF16),
                pltpu.VMEM((pl.cdiv(ctx, LANES), batch, LANES), F32),
                pltpu.VMEM((2, head, batch * LANES), BF16),
                pltpu.VMEM((2, half, width), F32),
                pltpu.VMEM((2, half, LANES), jnp.int32),
                pltpu.VMEM((2, 2, half, head), F32),
                sem((CHUNKS,)), sem, sem((4,)), sem((layers, 2)), sem((layers, 2)), sem((2 * layers,)),
                sem, sem, sem((2, n // 2, 2)), sem((2, n // 2, 2)),
                sem((2 * layers, 2, n)), sem((2 * layers, 2, n)), sem((layers, n)), sem((layers, n)), sem((layers, n)), sem((layers, n)),
                sem((2 * layers, n)), sem((2 * layers, n)),
                *[pltpu.VMEM(a.shape, a.dtype) for a in small],
                sem((SMALL,)),
            ],
            compiler_params=pltpu.CompilerParams(collective_id=0, has_side_effects=True, vmem_limit_bytes=STEP_VMEM),
            name="decode_step",
        )(
            *small,
            embed_table, pos_table, jnp.transpose(w_qkv[:, :, :, 0, :], (0, 2, 3, 1)), jnp.transpose(w_cq[:, :, 0, :], (0, 2, 1)),
            w_fc1, w_fc2, w_out[:, :, 0],
            by_place(self_keys), by_place(self_vals), by_place(cross_keys), by_place(cross_vals),
        )

        def in_vmem(a):
            return pltpu.with_memory_space_constraint(a, pltpu.VMEM)

        logits, new_keys, new_vals = pl.pallas_call(
            last_kernel,
            out_shape=(jax.ShapeDtypeStruct((batch, shard_rows), F32), jax.ShapeDtypeStruct(cache_rows, BF16), jax.ShapeDtypeStruct(cache_rows, BF16)),
            in_specs=[vmem] * 4,
            out_specs=(hbm, hbm, hbm),
            scratch_shapes=[pltpu.VMEM((batch, shard_rows), F32), sem((2, layers)), sem((3,))],
            compiler_params=pltpu.CompilerParams(vmem_limit_bytes=LAST_VMEM),
            name="last",
        )(in_vmem(final_hidden), in_vmem(table), in_vmem(sk), in_vmem(sv))

        def as_given(cache):
            return jnp.transpose(cache, (0, 1, 3, 2))[:, :, :, None, :]

        return logits, as_given(new_keys), as_given(new_vals)

    batch_spec = P("dp")
    cache_spec = P(None, "dp", None, "tp", None)
    in_specs = (batch_spec, batch_spec, cache_spec, cache_spec, cache_spec, cache_spec, P("tp", None), P(None, None), P(None, None, None, "tp", None), P(None, None, "tp", None), P(None, None, "tp", None), P(None, None, "tp", None, None), P(None, None, None), P(None, None, "tp"), P(None, "tp"), P(None, "tp", None), P(None, None, None, None), P(None, None))
    out_specs = (P("dp", "tp"), cache_spec, cache_spec)
    return jax.shard_map(local_step, mesh=mesh, in_specs=in_specs, out_specs=out_specs, check_vma=False)
```

```python
import functools

import jax
import jax.numpy as jnp
from jax import lax
from jax.experimental import pallas as pl
from jax.experimental.pallas import tpu as pltpu
from jax.sharding import PartitionSpec as P

MESH = pl.DeviceIdType.MESH
LANES = 128
GROUP = 4
CHUNKS = 8
SMALL = 7
STEP_VMEM = 42 * 1024 * 1024
LAST_VMEM = 8 * 1024 * 1024
F32 = jnp.float32
BF16 = jnp.bfloat16
NT = (((1,), (1,)), ((), ()))


def dot_nt(a, b):
    return lax.dot_general(a, b, NT, preferred_element_type=F32)


def dot_nn(a, b):
    return jnp.dot(a, b, preferred_element_type=F32)


def layer_norm(x, gain, shift):
    mean = jnp.mean(x, axis=-1, keepdims=True)
    centred = x - mean
    variance = jnp.mean(centred * centred, axis=-1, keepdims=True)
    return (centred * lax.rsqrt(variance + 1e-5) * gain + shift).astype(BF16)


def step_kernel(
    n, *refs,
):
    small_hbm, refs = refs[:SMALL], refs[SMALL:]
    (
    embed, pos_table, w_qkv_hbm, w_cq_hbm, fc1_hbm, fc2_hbm, w_out, self_k, self_v, cross_k, cross_v,
    final_out, table, sk, sv,
    ck, cv, wo_full, pos_vmem, w_qkv, w_cq, fc1, fc2, emb_own, emb_partner, emb_chip, emb_slots, o_slots,
    rs_src, rs_slots, ag_slots, one_hot, columns, x, places, fresh,
    sem_e, sem_p, sem_own, sem_self, sem_cross, sem_w, pair_send, pair_recv, emb_send, emb_recv,
    o_send, o_recv, rs_send, rs_recv, ag_send, ag_recv, w_send, w_recv,
    small, sem_small,
    ) = (*refs[:-SMALL - 1], refs[-SMALL - 1 : -1], refs[-1])
    tokens, positions, in_bias, out_bias, b_fc1, ln_layers, ln_final = small
    small_loads = [pltpu.make_async_copy(a, b, sem_small.at[i]) for i, (a, b) in enumerate(zip(small_hbm, small))]
    for c in small_loads:
        c.start()
    layers, batch = sk.shape[0], sk.shape[1]
    head, ctx = sk.shape[2], sk.shape[3]
    width = table.shape[1]
    half, block = batch // 2, width // (n // 2)
    me = lax.axis_index("tp")
    core, chip = lax.rem(me, 2), lax.div(me, 2)
    partner = me + 1 - 2 * core

    def peer(k):
        return lax.rem(me + k, n)

    barrier = pltpu.get_barrier_semaphore()
    for k in range(1, n):
        pl.semaphore_signal(barrier, 1, device_id={"tp": peer(k)}, device_id_type=MESH)

    chunks = sem_e.shape[0]
    chunk = table.shape[0] // chunks
    table_loads = [pltpu.make_async_copy(embed.at[pl.ds(c * chunk, chunk)], table.at[pl.ds(c * chunk, chunk)], sem_e.at[c]) for c in range(chunks)]
    for c in table_loads:
        c.start()
    pos_load = pltpu.make_async_copy(pos_table, pos_vmem, sem_p)
    pos_load.start()
    own = [pltpu.make_async_copy(a, b, sem_own.at[i]) for i, (a, b) in enumerate(((w_qkv_hbm, w_qkv), (w_cq_hbm, w_cq), (fc1_hbm, fc1), (fc2_hbm, fc2)))]
    self_loads = [[pltpu.make_async_copy(a.at[l], b.at[l], sem_self.at[l, i]) for i, (a, b) in enumerate(((self_k, sk), (self_v, sv)))] for l in range(layers)]
    key_loads = [pltpu.make_async_copy(cross_k.at[l], ck.at[l], sem_cross.at[l, 0]) for l in range(layers)]
    val_loads = [pltpu.make_async_copy(cross_v.at[l], cv, sem_cross.at[l, 1]) for l in range(layers)]
    later_loads = [own[0], *self_loads[0], *own[1:], key_loads[0], val_loads[0]]

    def remote(src, dst, send, recv, to):
        return pltpu.make_async_remote_copy(src, dst, send, recv, device_id={"tp": to}, device_id_type=MESH)

    order = sorted(range(1, n), key=lambda k: -min(k, n - k))

    def send_all(src_of, slots, send, recv):
        for k in order:
            remote(src_of(peer(k)), slots.at[me], send.at[k], recv.at[me], peer(k)).start()

    def wait_all(slots, send, recv):
        for k in order:
            j = peer(k)
            remote(slots.at[j], slots.at[j], send.at[k], recv.at[j], j).wait_recv()
        for k in order:
            remote(slots.at[me], slots.at[me], send.at[k], recv.at[me], peer(k)).wait_send()

    parts = [(w_out.at[l, a], wo_full.at[l, a]) for l in range(layers) for a in range(2)]
    own_copies, first_hop, second_hop = {}, {}, {}

    def weights_start(i):
        src, full = parts[i]
        own_copies[i] = pltpu.make_async_copy(src, full.at[me], sem_w.at[i])
        own_copies[i].start()
        first_hop[i] = [remote(src, full.at[me], w_send.at[i, k], w_recv.at[i, me], peer(k)) for k in range(2, n, 2)]
        first_hop[i].append(remote(src, full.at[me], w_send.at[i, 1], w_recv.at[i, me], partner))
        for c in first_hop[i]:
            c.start()

    def weights_forward(i):
        src, full = parts[i]
        second_hop[i] = []
        for k in range(2, n, 2):
            j = peer(k)
            remote(src, full.at[j], w_send.at[i, k], w_recv.at[i, j], j).wait_recv()
            c = remote(full.at[j], full.at[j], w_send.at[i, k + 1], w_recv.at[i, j], partner)
            c.start()
            second_hop[i].append(c)

    def weights_wait(i):
        src, full = parts[i]
        remote(src, full.at[partner], w_send.at[i, 1], w_recv.at[i, partner], partner).wait_recv()
        for k in range(2, n, 2):
            j = lax.rem(partner + k, n)
            remote(src, full.at[j], w_send.at[i, k + 1], w_recv.at[i, j], partner).wait_recv()
        for c in first_hop[i] + second_hop[i]:
            c.wait_send()
        own_copies[i].wait()

    def as_column(row):
        i = lax.broadcasted_iota(jnp.int32, (batch, batch), 0)
        j = lax.broadcasted_iota(jnp.int32, (batch, batch), 1)
        return jnp.sum(jnp.where(i == j, jnp.broadcast_to(row.astype(F32), (batch, batch)), 0.0), axis=1, keepdims=True)

    for c in small_loads:
        c.wait()
    token = as_column(tokens[...]).astype(jnp.int32) - me * table.shape[0]
    place = as_column(positions[...]).astype(jnp.int32)
    pl.semaphore_wait(barrier, n - 1)
    weights_start(0)
    picked = jnp.zeros((batch, width), F32)
    for c in range(chunks):
        table_loads[c].wait()
        hit = lax.broadcasted_iota(jnp.int32, (batch, chunk), 1) + c * chunk == token
        picked = picked + dot_nn(jnp.where(hit, 1.0, 0.0).astype(BF16), table[c * chunk : (c + 1) * chunk])
    for c in later_loads:
        c.start()
    emb_own[...] = picked.astype(BF16)

    pair = remote(emb_own, emb_partner, pair_send, pair_recv, partner)
    pair.start()
    hit = lax.broadcasted_iota(jnp.int32, (batch, ctx), 1) == place
    hit = jnp.where(hit, 1.0, 0.0)
    for t in range(0, ctx, LANES):
        size = min(LANES, ctx - t)
        one_hot[t // LANES, :, :size] = hit[:, t : t + size]
    pos_load.wait()
    pos_rows = dot_nn(hit.astype(BF16), pos_vmem[...])
    pair.wait()
    pair_sum = picked + emb_partner[...].astype(F32)
    for r in range(2):
        emb_chip[r] = pair_sum[r * half : (r + 1) * half].astype(BF16)
    cols = width // 2
    distances = (n // 4, *[d for d in range(1, n // 2) if d != n // 4])

    def table_hop(dc, other, r):
        to = lax.rem(chip + dc, n // 2) * 2 + lax.rem(core + other, 2)
        here = pl.ds(pl.multiple_of(core * cols, LANES), cols)
        return remote(emb_chip.at[r, :, here], emb_slots.at[chip, r, :, here], emb_send.at[r, dc, other], emb_recv.at[r, chip, core], to)

    for r in range(2):
        for dc in distances:
            for other in range(2):
                table_hop(dc, other, r).start()
    weights_start(1)
    for r in range(2):
        x[r] = pair_sum[r * half : (r + 1) * half] + pos_rows[r * half : (r + 1) * half]
        places[r] = jnp.broadcast_to(place[r * half : (r + 1) * half], (half, LANES))

    def table_stage(r):
        total = x[r]
        for dc in reversed(distances):
            far = lax.rem(chip + dc, n // 2)
            for c in range(2):
                slot = emb_slots.at[far, r, :, c * cols : (c + 1) * cols]
                remote(slot, slot, emb_send.at[r, dc, c], emb_recv.at[r, far, c], far * 2 + c).wait_recv()
            total = total + emb_slots[far, r].astype(F32)
        x[r] = total

    def table_sent():
        for r in range(2):
            for dc in distances:
                for other in range(2):
                    table_hop(dc, other, r).wait_send()

    span = GROUP * head
    diagonal = lax.broadcasted_iota(jnp.int32, (GROUP, span), 0) == lax.div(lax.broadcasted_iota(jnp.int32, (GROUP, span), 1), head)

    def attend(q, keys, vals, finish):
        length = keys.shape[2]
        q = q.astype(F32)
        groups = [slice(g, g + GROUP) for g in range(0, half, GROUP)]
        wide = [jnp.where(diagonal, jnp.concatenate([q[rows]] * GROUP, axis=1), 0.0).astype(BF16) for rows in groups]
        scores = [dot_nn(w, keys[rows].reshape(span, length)) for w, rows in zip(wide, groups)]
        finished = [finish(s * (head ** -0.5), rows) for s, rows in zip(scores, groups)]
        out = []
        for (weights, extra), rows in zip(finished, groups):
            full = jnp.where(diagonal, dot_nt(weights, vals[rows].reshape(span, length)), 0.0)
            total = full[:, :LANES]
            for c in range(LANES, span, LANES):
                total = total + full[:, c : c + LANES]
            mixed = total[:, :head]
            for c in range(head, LANES, head):
                mixed = mixed + total[:, c : c + head]
            out.append(mixed + extra)
        return jnp.concatenate(out, axis=0)

    def head_slots(e, r):
        return o_slots.at[e, r], o_send.at[e, r], o_recv.at[e, r]

    def exchange_heads(e, r, attended):
        slots, send, recv = head_slots(e, r)
        slots[me] = attended.astype(BF16)
        send_all(lambda j: slots.at[me], slots, send, recv)

    def project(l, a, r):
        slots, send, recv = head_slots(2 * l + a, r)
        total = dot_nn(slots[me], wo_full[l, a, me])
        for k in reversed(order):
            j = peer(k)
            remote(slots.at[j], slots.at[j], send.at[k], recv.at[j], j).wait_recv()
            total = total + dot_nn(slots[j], wo_full[l, a, j])
        for k in order:
            remote(slots.at[me], slots.at[me], send.at[k], recv.at[me], peer(k)).wait_send()
        return total.astype(BF16).astype(F32)

    def put_columns(l):
        eye = (lax.broadcasted_iota(jnp.int32, (head, head), 0) == lax.broadcasted_iota(jnp.int32, (head, head), 1))
        eye = jnp.where(eye, 1.0, 0.0).astype(BF16)
        wide = batch * LANES
        spread = lax.broadcasted_iota(jnp.int32, (batch, wide), 0) == lax.div(lax.broadcasted_iota(jnp.int32, (batch, wide), 1), LANES)
        spread = jnp.where(spread, 1.0, 0.0).astype(BF16)
        for i in range(2):
            rows = jnp.concatenate([fresh[i, 0], fresh[i, 1]], axis=0).astype(BF16)
            columns[i] = dot_nn(dot_nt(eye, rows).astype(BF16), spread).astype(BF16)

        def one(b, carry):
            for t in range(0, ctx, LANES):
                size = min(LANES, ctx - t)
                here = jnp.broadcast_to(one_hot[t // LANES, pl.ds(b, 1), :], (head, LANES))[:, :size].astype(BF16) > 0.5
                for i, cache in enumerate((sk, sv)):
                    fresh = columns[i, :, pl.ds(pl.multiple_of(b * LANES, LANES), LANES)][:, :size]
                    cache[l, b, :, t : t + size] = jnp.where(here, fresh, cache[l, b, :, t : t + size])
            return carry

        lax.fori_loop(0, batch, one, 0)

    def self_stage(l, r):
        ln = ln_layers[l]
        rows = pl.ds(r * half, half)
        h = layer_norm(x[r], ln[0, 0:1], ln[0, 1:2])
        q = (dot_nt(h, w_qkv[l, 0]) + in_bias[l, 0]).astype(BF16)
        k_new = dot_nt(h, w_qkv[l, 1]).astype(BF16)
        v_new = (dot_nt(h, w_qkv[l, 2]) + in_bias[l, 1]).astype(BF16)
        fresh[0, r] = k_new.astype(F32)
        fresh[1, r] = v_new.astype(F32)
        here = places[r][:, :1]
        all_new = jnp.sum(q.astype(F32) * k_new.astype(F32), axis=-1, keepdims=True) * (head ** -0.5)

        def finish(s, rows):
            new_score = all_new[rows]
            s = jnp.where(lax.broadcasted_iota(jnp.int32, s.shape, 1) < here[rows], s, -1e30)
            peak = jnp.maximum(jnp.max(s, axis=-1, keepdims=True), new_score)
            e = jnp.exp(s - peak)
            e_new = jnp.exp(new_score - peak)
            total = jnp.sum(e, axis=-1, keepdims=True) + e_new
            return (e / total).astype(BF16), (e_new / total).astype(BF16).astype(F32) * v_new.astype(F32)[rows]

        attended = attend(q, sk.at[l, rows], sv.at[l, rows], finish)
        exchange_heads(2 * l, r, attended)

    def cross_stage(l, r):
        ln = ln_layers[l]
        rows = pl.ds(r * half, half)
        x[r] = x[r] + project(l, 0, r) + out_bias[0, l : l + 1]
        h = layer_norm(x[r], ln[1, 0:1], ln[1, 1:2])
        q = (dot_nt(h, w_cq[l]) + in_bias[l, 2]).astype(BF16)

        def finish(s, rows):
            e = jnp.exp(s - jnp.max(s, axis=-1, keepdims=True))
            return (e / jnp.sum(e, axis=-1, keepdims=True)).astype(BF16), 0.0

        attended = attend(q, ck.at[l, rows], cv.at[rows], finish)
        exchange_heads(2 * l + 1, r, attended)

    def mlp_stage(l, r):
        ln = ln_layers[l]
        x[r] = x[r] + project(l, 1, r) + out_bias[1, l : l + 1]
        h = layer_norm(x[r], ln[2, 0:1], ln[2, 1:2])
        hidden = dot_nn(h, fc1[l]) + b_fc1[l : l + 1]
        active = (0.5 * hidden * (1.0 + lax.erf(hidden * (0.5 ** 0.5)))).astype(BF16)
        partial = dot_nn(active, fc2[l])
        for c in range(n // 2):
            rs_src[l, r * (n // 2) + c] = partial[:, c * block : (c + 1) * block]
        for k in order:
            pl.when(lax.div(peer(k), n // 2) == r)(rs_copy(l, k).start)

    def rs_copy(l, k):
        j = peer(k)
        return remote(rs_src.at[l, j], rs_slots.at[l, me], rs_send.at[l, k], rs_recv.at[l, me], j)

    def sum_stage(l):
        wait_all(rs_slots.at[l], rs_send.at[l], rs_recv.at[l])
        rs_slots[l, me] = rs_src[l, me]
        total = rs_slots[l, 0]
        for j in range(1, n):
            total = total + rs_slots[l, j]
        ag_slots[l, me] = total.astype(BF16)
        send_all(lambda j: ag_slots.at[l, me], ag_slots.at[l], ag_send.at[l], ag_recv.at[l])

    def add_stage(l, r):
        for k in order:
            j = peer(k)
            slot = ag_slots.at[l, j]
            pl.when(lax.div(j, n // 2) == r)(remote(slot, slot, ag_send.at[l, k], ag_recv.at[l, j], j).wait_recv)
        x[r] = x[r] + jnp.concatenate([ag_slots[l, r * (n // 2) + c].astype(F32) for c in range(n // 2)], axis=1) + out_bias[2, l : l + 1]

    def both(stage, l):
        def one(r, carry):
            stage(l, r)
            return carry

        lax.fori_loop(0, 2, one, 0)

    def sent(l):
        for k in order:
            remote(ag_slots.at[l, me], ag_slots.at[l, me], ag_send.at[l, k], ag_recv.at[l, me], peer(k)).wait_send()

    def first_stage(l, r):
        table_stage(r)
        self_stage(l, r)

    def next_stage(l, r):
        add_stage(l - 1, r)
        self_stage(l, r)

    def end_stage(l, r):
        add_stage(l - 1, r)
        final_out[pl.ds(pl.multiple_of(r * half, half), half)] = layer_norm(x[r], ln_final[0:1], ln_final[1:2])

    own[0].wait()
    for c in self_loads[0]:
        c.wait()
    both(first_stage, 0)
    table_sent()
    for l in range(layers):
        last = l + 1 == layers
        weights_forward(2 * l)
        if l == 0:
            for c in own[1:]:
                c.wait()
        weights_wait(2 * l)
        key_loads[l].wait()
        val_loads[l].wait()
        if not last:
            for c in (*self_loads[l + 1], key_loads[l + 1]):
                c.start()
        both(cross_stage, l)
        if not last:
            val_loads[l + 1].start()
            weights_start(2 * l + 2)
        weights_forward(2 * l + 1)
        weights_wait(2 * l + 1)
        both(mlp_stage, l)
        if not last:
            weights_start(2 * l + 3)
        put_columns(l)
        sum_stage(l)
        if not last:
            for c in self_loads[l + 1]:
                c.wait()
            both(next_stage, l + 1)
        else:
            both(end_stage, l + 1)
        sent(l)


def last_kernel(final, table, sk, sv, logits_out, keys_out, vals_out, logits, sems, logit_sems):
    copies = []
    for i, (src, dst) in enumerate(((sk, keys_out), (sv, vals_out))):
        for l in range(sk.shape[0]):
            copies.append(pltpu.make_async_copy(src.at[l], dst.at[l], sems.at[i, l]))
            copies[-1].start()
    h = final[...]
    pieces = logit_sems.shape[0]
    piece = logits.shape[1] // pieces
    for c in range(pieces):
        here = pl.ds(c * piece, piece)
        logits[:, here] = dot_nt(h, table[here, :])
        copies.append(pltpu.make_async_copy(logits.at[:, here], logits_out.at[:, here], logit_sems.at[c]))
        copies[-1].start()
    for c in copies:
        c.wait()


def solution(mesh):
    n = mesh.shape["tp"]

    def local_step(tokens, positions, self_keys, self_vals, cross_keys, cross_vals, embed_table, pos_table, w_qkv, w_cq, in_bias, w_out, out_bias, w_fc1, b_fc1, w_fc2, ln_layers, ln_final):
        layers, batch, ctx, _, head = self_keys.shape
        frames = cross_keys.shape[2]
        shard_rows, width = embed_table.shape
        hidden = w_fc1.shape[2]
        half, block = batch // 2, width // (n // 2)

        def by_place(cache):
            return jnp.transpose(cache[:, :, :, 0, :], (0, 1, 3, 2))

        vmem = pl.BlockSpec(memory_space=pltpu.VMEM)
        hbm = pl.BlockSpec(memory_space=pl.ANY)
        sem = pltpu.SemaphoreType.DMA
        cache_rows = (layers, batch, head, ctx)
        small = (tokens[None], positions[None], in_bias, jnp.transpose(out_bias, (1, 0, 2)), b_fc1, ln_layers, ln_final)
        final_hidden, table, sk, sv = pl.pallas_call(
            functools.partial(step_kernel, n),
            out_shape=(pltpu.VMEM((batch, width), BF16), pltpu.VMEM((shard_rows, width), BF16), pltpu.VMEM(cache_rows, BF16), pltpu.VMEM(cache_rows, BF16)),
            in_specs=[hbm] * (SMALL + 11),
            out_specs=(vmem, vmem, vmem, vmem),
            scratch_shapes=[
                pltpu.VMEM((layers, batch, head, frames), BF16),
                pltpu.VMEM((batch, head, frames), BF16),
                pltpu.VMEM((layers, 2, n, head, width), BF16),
                pltpu.VMEM(pos_table.shape, BF16),
                pltpu.VMEM((layers, 3, head, width), BF16),
                pltpu.VMEM((layers, head, width), BF16),
                pltpu.VMEM(w_fc1.shape, BF16),
                pltpu.VMEM(w_fc2.shape, BF16),
                pltpu.VMEM((batch, width), BF16),
                pltpu.VMEM((batch, width), BF16),
                pltpu.VMEM((2, half, width), BF16),
                pltpu.VMEM((n // 2, 2, half, width), BF16),
                pltpu.VMEM((2 * layers, 2, n, half, head), BF16),
                pltpu.VMEM((layers, n, half, block), F32),
                pltpu.VMEM((layers, n, half, block), F32),
                pltpu.VMEM((layers, n, half, block), BF16),
                pltpu.VMEM((pl.cdiv(ctx, LANES), batch, LANES), F32),
                pltpu.VMEM((2, head, batch * LANES), BF16),
                pltpu.VMEM((2, half, width), F32),
                pltpu.VMEM((2, half, LANES), jnp.int32),
                pltpu.VMEM((2, 2, half, head), F32),
                sem((CHUNKS,)), sem, sem((4,)), sem((layers, 2)), sem((layers, 2)), sem((2 * layers,)),
                sem, sem, sem((2, n // 2, 2)), sem((2, n // 2, 2)),
                sem((2 * layers, 2, n)), sem((2 * layers, 2, n)), sem((layers, n)), sem((layers, n)), sem((layers, n)), sem((layers, n)),
                sem((2 * layers, n)), sem((2 * layers, n)),
                *[pltpu.VMEM(a.shape, a.dtype) for a in small],
                sem((SMALL,)),
            ],
            compiler_params=pltpu.CompilerParams(collective_id=0, has_side_effects=True, vmem_limit_bytes=STEP_VMEM),
            name="decode_step",
        )(
            *small,
            embed_table, pos_table, jnp.transpose(w_qkv[:, :, :, 0, :], (0, 2, 3, 1)), jnp.transpose(w_cq[:, :, 0, :], (0, 2, 1)),
            w_fc1, w_fc2, w_out[:, :, 0],
            by_place(self_keys), by_place(self_vals), by_place(cross_keys), by_place(cross_vals),
        )

        def in_vmem(a):
            return pltpu.with_memory_space_constraint(a, pltpu.VMEM)

        logits, new_keys, new_vals = pl.pallas_call(
            last_kernel,
            out_shape=(jax.ShapeDtypeStruct((batch, shard_rows), F32), jax.ShapeDtypeStruct(cache_rows, BF16), jax.ShapeDtypeStruct(cache_rows, BF16)),
            in_specs=[vmem] * 4,
            out_specs=(hbm, hbm, hbm),
            scratch_shapes=[pltpu.VMEM((batch, shard_rows), F32), sem((2, layers)), sem((3,))],
            compiler_params=pltpu.CompilerParams(vmem_limit_bytes=LAST_VMEM),
            name="last",
        )(in_vmem(final_hidden), in_vmem(table), in_vmem(sk), in_vmem(sv))

        def as_given(cache):
            return jnp.transpose(cache, (0, 1, 3, 2))[:, :, :, None, :]

        return logits, as_given(new_keys), as_given(new_vals)

    batch_spec = P("dp")
    cache_spec = P(None, "dp", None, "tp", None)
    in_specs = (batch_spec, batch_spec, cache_spec, cache_spec, cache_spec, cache_spec, P("tp", None), P(None, None), P(None, None, None, "tp", None), P(None, None, "tp", None), P(None, None, "tp", None), P(None, None, "tp", None, None), P(None, None, None), P(None, None, "tp"), P(None, "tp"), P(None, "tp", None), P(None, None, None, None), P(None, None))
    out_specs = (P("dp", "tp"), cache_spec, cache_spec)
    return jax.shard_map(local_step, mesh=mesh, in_specs=in_specs, out_specs=out_specs, check_vma=False)
```
